32 devices in a mesh: dp: 8 (over z, x), mp: 4 (over y, core).
Axes of the slice: x: 2, y: 2, z: 4, core: 2. Of those that a mesh axis runs over, the one named last changes fastest.
Arguments:
- patches: bfloat16 [4096, 2048], P('dp'), may hold values from -6 to 6
- cotangent: bfloat16 [4096, 8192], P('dp', 'mp'), may hold values from -0.09375 to 0.09375
- weight: float32 [2048, 8192], P('dp', 'mp'), may hold values from -0.125 to 0.125
- accum: float32 [2048, 8192], P('dp', 'mp'), may hold values from 0.1 to 4
Outputs:
- new_weight: float32 [2048, 8192], P(('dp', 'mp'))
- new_accum: float32 [2048, 8192], P(('dp', 'mp'))
- weight_copy: bfloat16 [2048, 8192], P(None, 'mp')
The draws below stay inside these ranges and needn't reach their ends.
All inputs are finite; a program needn't handle non-finite values.
Results may differ from the reference program's by a relative error of at most 0.001.
Values may be sent and summed in bfloat16 or wider, within the bound.
A program may use at most 192 MiB of HBM per device.

```python
import math
import jax
import jax.numpy as jnp
from jax import lax

D = 2048
FF = 8192
TOKENS = 4096


def spiked(entries, rng, source, target, blocks, factor):
    def block_of(position):
        return (jnp.arange(entries.shape[position]) // (entries.shape[position] // blocks)).reshape((-1,) + (1,) * (entries.ndim - 1 - position))

    one_side = jax.random.permutation(rng, blocks)[block_of(target)]
    far = (block_of(target) + blocks // 2) % blocks
    return jnp.where((block_of(source) == one_side) | (block_of(source) == far), factor * entries, entries)


def block_levels(rng, dims, shards, low, largest):
    def one(position, parts):
        heights = jax.random.uniform(jax.random.fold_in(jax.random.fold_in(rng, 6), position), (parts,), jnp.float32, low / len(shards), largest / len(shards))
        return jnp.repeat(jnp.exp(heights), dims[position] // parts).reshape((-1,) + (1,) * (len(dims) - position - 1))

    loudness = one(*shards[0])
    for cut in shards[1:]:
        loudness = loudness * one(*cut)
    return loudness


def noise(stream_key, shape, width, bound, shards=(), held_as=jnp.bfloat16):
    result = jax.random.normal(stream_key, shape, jnp.float32) * width
    if len(shards) > 0:
        result = block_levels(stream_key, shape, shards, -0.22, 0.18) * result
    return jnp.clip(result, min=-bound, max=bound).astype(held_as)


def noise_with(rng, extent, spread, bound, pieces, heavy, held_as=jnp.bfloat16):
    values = spread * jax.random.normal(rng, extent, jnp.float32)
    if pieces:
        values = values * block_levels(rng, extent, pieces, -0.22, 0.18)
    return jnp.clip(spiked(values, jax.random.fold_in(rng, 3), *heavy), -bound, bound).astype(held_as)


def setup_inputs(seed: int = 0) -> dict:
    key_of = jax.random.split(jax.random.key(seed), 5)
    return {
        "patches": noise_with(key_of[0], (TOKENS, D), 1.0, 6.0, ((0, 8),), (0, 1, 8, 2.0)),
        "cotangent": noise(key_of[1], (TOKENS, FF), TOKENS ** -0.5, 0.09375, ((0, 8), (1, 4))),
        "weight": noise(key_of[2], (D, FF), D ** -0.5, 0.125, ((0, 8), (1, 4)), jnp.float32),
        "accum": jnp.clip(jnp.exp(math.log(4.0) - 3.6888794 * jax.random.uniform(key_of[3], (D, FF), jnp.float32) ** block_levels(key_of[3], (D, FF), ((0, 8), (1, 4)), -0.2, 0.2)), 0.1, 4.0),
    }


learning_rate = 0.02

def reference(patches, cotangent, weight, accum):
    grad = jnp.dot(patches.T, cotangent, preferred_element_type=jnp.float32)
    new_accum = accum + grad * grad
    new_weight = weight - learning_rate * grad * lax.rsqrt(new_accum)
    weight_copy = new_weight.astype(jnp.bfloat16)
    return (new_weight, new_accum, weight_copy)
```

```python
import functools

import jax
import jax.numpy as jnp
from jax import lax
from jax.experimental import pallas as pl
from jax.experimental.pallas import tpu as pltpu
from jax.sharding import PartitionSpec as P

learning_rate = 0.02
largest_product = 0.5625
power = 7
lag = 1


def kernel(a, b, m, direct, wide, scale, p_ref, t_ref, w_ref, s_ref, ow_ref, os_ref, oc_ref,
           pv, pt, tv, wv, sv, cv, gv, rbuf, sbuf,
           fown, fsend, frecv, qsend, qrecv, tsem, lsem, rsend, rrecv, csend, crecv, xsend, xrecv, msend, mrecv, osem):
    nc, _, cc = tv.shape
    rows, full = w_ref.shape
    tok = tv.shape[1] // b
    part_tok = tok // m
    sub = rows // m
    me = lax.axis_index("dp")
    mi = lax.axis_index("mp")
    zi = lax.div(me, b)
    xi = lax.rem(me, b)
    has_left = zi > 0
    has_right = zi < a - 1

    def inner(j):
        return lax.rem(xi + j, b)

    def peer(j):
        return {"dp": zi * b + inner(j)}

    def other(j):
        return lax.rem(mi + j, m)

    left, right = {"dp": me - b}, {"dp": me + b}

    def remote(src, dst, send, recv, device):
        return pltpu.make_async_remote_copy(
            src_ref=src, dst_ref=dst, send_sem=send, recv_sem=recv,
            device_id=device, device_id_type=pl.DeviceIdType.MESH)

    def cols(c):
        return pl.ds(pl.multiple_of(c * cc, cc), cc)

    def block(i):
        return pl.ds(pl.multiple_of(i * rows, rows), rows)

    def span(start, size):
        return pl.ds(pl.multiple_of(start, size), size)

    def features(i, q=None):
        toks = slice(None) if q is None else span(q * part_tok, part_tok)
        return p_ref.at[toks, block(i)] if direct else p_ref.at[block(i), toks]

    def gathered(d, x, q=None):
        if direct:
            return pv.at[d, x] if q is None else pv.at[d, x, span(q * part_tok, part_tok)]
        return pt.at[d, :, span(x * tok, tok)] if q is None else pt.at[d, :, span(x * tok + q * part_tok, part_tok)]

    def own_features(d):
        return pltpu.make_async_copy(features(d * b + xi), gathered(d, xi), fown.at[d])

    def send_features(d, j):
        return remote(features(d * b + inner(j), mi), gathered(d, xi, mi), fsend.at[d, j], frecv.at[d, j], peer(j))

    def recv_features(d, j):
        return remote(features(d * b + xi, mi), gathered(d, inner(b - j), mi), fsend.at[d, j], frecv.at[d, j], peer(j))

    def relay_features(d, j, k):
        spot = gathered(d, inner(b - j), mi)
        return remote(spot, spot, qsend.at[d, j, k], qrecv.at[d, j, k], {"mp": other(k)})

    def recv_relay(d, j, k):
        spot = gathered(d, inner(b - j), other(m - k))
        return remote(spot, spot, qsend.at[d, j, k], qrecv.at[d, j, k], {"mp": other(k)})

    def tokens_at(c, x):
        return tv.at[c, span(x * tok, tok)]

    def own_tokens(c):
        return pltpu.make_async_copy(t_ref.at[:, cols(c)], tokens_at(c, xi), lsem.at[0, c])

    def own_weight(c):
        return pltpu.make_async_copy(w_ref.at[:, cols(c)], wv.at[c], lsem.at[1, c])

    def own_accum(c):
        return pltpu.make_async_copy(s_ref.at[:, cols(c)], sv.at[c], lsem.at[2, c])

    def send_tokens(c, j):
        return remote(t_ref.at[:, cols(c)], tokens_at(c, xi), tsem.at[0, c, j], tsem.at[1, c, j], peer(j))

    def recv_tokens(c, j):
        return remote(t_ref.at[:, cols(c)], tokens_at(c, inner(b - j)), tsem.at[0, c, j], tsem.at[1, c, j], peer(j))

    def pass_sum(side, c, d):
        return remote(sbuf.at[c, d], rbuf.at[side, c, d], rsend.at[c, d], rrecv.at[side, c, d],
                      right if side == 0 else left)

    def region(owner, c):
        return oc_ref.at[block(owner), cols(c)]

    def pass_copy(side, c, h, owner_z, j, src=None):
        spot = region(owner_z * b + inner(j), c)
        return remote(spot if src is None else src, spot, csend.at[side, c, h, j], crecv.at[side, c, h, j],
                      right if side == 0 else left)

    def share_copy(c, z, j, src=None):
        spot = region(z * b + xi, c)
        return remote(spot if src is None else src, spot, xsend.at[c, z, j], xrecv.at[c, z, j], peer(j))

    def recv_share(c, z, j):
        spot = region(z * b + inner(b - j), c)
        return remote(spot, spot, xsend.at[c, z, j], xrecv.at[c, z, j], peer(j))

    def flat(c, k, src_dev):
        ref = ow_ref if k == 0 else os_ref
        return ref.at[:, span(src_dev * full + c * cc, cc)]

    def part(c, k, i):
        v = wv if k == 0 else sv
        return v.at[c, span(i * sub, sub)]

    def send_flat(c, k, j):
        return remote(part(c, k, other(j)), flat(c, k, mi), msend.at[c, k, j], mrecv.at[c, k, j], {"mp": other(j)})

    def recv_flat(c, k, j):
        return remote(part(c, k, mi), flat(c, k, other(m - j)), msend.at[c, k, j], mrecv.at[c, k, j], {"mp": other(j)})

    def own_flat(c, k):
        return pltpu.make_async_copy(part(c, k, mi), flat(c, k, mi), osem.at[c, k])

    def own_copy(c):
        return pltpu.make_async_copy(cv.at[c], region(me, c), osem.at[c, 2])

    def across_first(c):
        return lax.rem(c * wide, 16) >= 16 - wide

    def valid(c):
        return (c >= 0) & (c < nc)

    barrier = pltpu.get_barrier_semaphore()

    def greet(device):
        pl.semaphore_signal(barrier, inc=1, device_id=device, device_id_type=pl.DeviceIdType.MESH)

    for j in range(1, b):
        greet(peer(j))
    for j in range(1, m):
        greet({"mp": other(j)})
    pl.when(has_left)(lambda: greet(left))
    pl.when(has_right)(lambda: greet(right))

    for d in range(a):
        own_features(d).start()

    @pl.loop(0, nc)
    def _(c):
        own_tokens(c).start()
        own_weight(c).start()
        own_accum(c).start()

    pl.semaphore_wait(barrier, b - 1 + m - 1 + jnp.minimum(zi, 1) + jnp.minimum(a - 1 - zi, 1))

    def in_order(do):
        for k in range(a):
            pl.when(a - 1 - k > zi)(functools.partial(do, a - 1 - k))
            pl.when(k < zi)(functools.partial(do, k))
        do(zi)

    def start_features(d):
        for j in range(1, b):
            send_features(d, j).start()

    for j in range(1, b):
        send_tokens(0, j).start()
    in_order(start_features)

    @pl.loop(1, nc)
    def _(c):
        for j in range(1, b):
            send_tokens(c, j).start()

    def spread_features(d):
        for j in range(1, b):
            recv_features(d, j).wait_recv()
            for k in range(1, m):
                relay_features(d, j, k).start()

    in_order(spread_features)

    def product(c, d):
        return jnp.dot(pt[d], tv[c], preferred_element_type=jnp.float32)

    def coded(v):
        v = v * scale
        square = v * v
        return (square * square * square * v).astype(jnp.bfloat16)

    def decoded(code):
        c = code.astype(jnp.float32)
        size = jnp.maximum(jnp.abs(c), 2.0 ** -126)
        return c * jnp.exp2(jnp.log2(size) * (1 / power - 1)) * (1 / scale)

    def features_here(d):
        own_features(d).wait()
        for j in range(1, b):
            for k in range(1, m):
                recv_relay(d, j, k).wait_recv()
        if direct:
            for x in range(b):
                pt[d, :, x * tok:(x + 1) * tok] = pv[d, x].T

    def stage_tokens(c):
        own_tokens(c).wait()
        for j in range(1, b):
            recv_tokens(c, j).wait_recv()

    def stage_sums(side, c):
        count, fed = (a - 1 - zi, has_left) if side == 0 else (zi, has_right)

        @pl.loop(0, count)
        def _(k):
            d = a - 1 - k if side == 0 else k
            pl.when(c == 0)(lambda: features_here(d))

            @pl.when(fed)
            def _():
                total = product(c, d)
                pass_sum(side, c, d).wait_recv()
                sbuf[c, d] = coded(total + decoded(rbuf[side, c, d]))

            @pl.when(jnp.logical_not(fed))
            def _():
                sbuf[c, d] = coded(product(c, d))

            pass_sum(side, c, d).start()

    def stage_update(c):
        pl.when(c == 0)(lambda: features_here(zi))
        gv[...] = product(c, zi)
        for side, there in ((0, has_left), (1, has_right)):
            @pl.when(there)
            def _(side=side):
                pass_sum(side, c, zi).wait_recv()
                gv[...] += decoded(rbuf[side, c, zi])
        own_weight(c).wait()
        own_accum(c).wait()
        grad = gv[...]
        summed = sv[c] + grad * grad
        weight = wv[c] - learning_rate * grad * lax.rsqrt(summed)
        cv[c] = weight.astype(cv.dtype)
        sv[c] = summed
        wv[c] = weight
        pl.when(has_right)(lambda: pass_copy(0, c, 0, zi, 0, cv.at[c]).start())
        pl.when(has_left)(lambda: pass_copy(1, c, 0, zi, 0, cv.at[c]).start())
        for j in range(1, b):
            share_copy(c, zi, j, cv.at[c]).start()
        own_copy(c).start()
        for k in range(2):
            for j in range(1, m):
                send_flat(c, k, j).start()
            own_flat(c, k).start()

    def stage_across(c):
        for j in range(1, b):
            recv_share(c, zi, b - j).wait_recv()
            pl.when(has_right)(lambda: pass_copy(0, c, 0, zi, j).start())
            pl.when(has_left)(lambda: pass_copy(1, c, 0, zi, j).start())

    def distance(z):
        return jnp.maximum(z, a - 1 - z) * lag

    @pl.loop(0, nc + (2 * (a - 1) + 1) * lag)
    def _(i):
        ready = i - jnp.minimum(zi, a - 1 - zi) * lag
        pl.when(valid(ready))(lambda: stage_tokens(ready))
        going_right = i - zi * lag
        pl.when(valid(going_right))(lambda: stage_sums(0, going_right))
        going_left = i - (a - 1 - zi) * lag
        pl.when(valid(going_left))(lambda: stage_sums(1, going_left))
        mine = i - distance(zi)
        pl.when(valid(mine))(lambda: stage_update(mine))
        if wide:
            before = mine - lag
            pl.when(valid(before) & across_first(before))(lambda: stage_across(before))
        for h in range(1, a):
            for side in range(2):
                owner_z = zi - h if side == 0 else zi + h
                there = owner_z >= 0 if side == 0 else owner_z < a
                further = has_right if side == 0 else has_left
                c = i - distance(owner_z) - h * lag

                @pl.when(there & valid(c))
                def _(side=side, h=h, c=c, owner_z=owner_z, further=further):
                    pass_copy(side, c, h - 1, owner_z, 0).wait_recv()
                    pl.when(further)(lambda: pass_copy(side, c, h, owner_z, 0).start())

                    @pl.when(jnp.logical_not(across_first(c)))
                    def _():
                        for j in range(1, b):
                            share_copy(c, owner_z, j).start()

                if wide:
                    e = c - lag

                    @pl.when(there & valid(e) & across_first(e))
                    def _(side=side, h=h, e=e, owner_z=owner_z, further=further):
                        for j in range(1, b):
                            pass_copy(side, e, h - 1, owner_z, j).wait_recv()
                            pl.when(further)(lambda: pass_copy(side, e, h, owner_z, j).start())

    for d in range(a):
        for j in range(1, b):
            send_features(d, j).wait_send()
            for k in range(1, m):
                relay_features(d, j, k).wait_send()

    @pl.loop(0, nc)
    def _(c):
        straight = jnp.logical_not(across_first(c))
        for j in range(1, b):
            send_tokens(c, j).wait_send()
            for z in range(a):
                pl.when((z == zi) | straight)(lambda: share_copy(c, z, j).wait_send())
                pl.when(straight)(lambda: recv_share(c, z, j).wait_recv())
        for d in range(a):
            pl.when(d != zi)(lambda: pass_sum(0, c, d).wait_send())
        for h in range(a - 1):
            for side, owned, further in ((0, zi >= h, has_right), (1, zi + h < a, has_left)):
                pl.when(owned & further)(lambda: pass_copy(side, c, h, zi, 0).wait_send())
                if wide:
                    @pl.when(owned & further & across_first(c))
                    def _():
                        for j in range(1, b):
                            pass_copy(side, c, h, zi, j).wait_send()
        own_copy(c).wait()
        for k in range(2):
            for j in range(1, m):
                send_flat(c, k, j).wait_send()
                recv_flat(c, k, j).wait_recv()
            own_flat(c, k).wait()


def shards(n, m, patches, cotangent, weight, accum):
    a = 1
    while a * a < n:
        a *= 2
    b = n // a
    nc = 16 if b == 2 else 8
    wide = 4 if b == 2 else 0
    direct = weight.shape[0] % 128 == 0
    tok, dim = patches.shape
    rows, full = weight.shape
    cc = full // nc
    columns = b if wide else 1
    scale = 1.0
    while (2 * scale * largest_product * tok * n) ** power < 2.0 ** 125:
        scale *= 2
    while (scale * largest_product * tok * n) ** power >= 2.0 ** 125:
        scale /= 2
    f32, bf16 = jnp.float32, jnp.bfloat16
    dma = pltpu.SemaphoreType.DMA
    flops = 2 * tok * b * a * rows * full
    return pl.pallas_call(
        functools.partial(kernel, a, b, m, direct, wide, scale),
        out_shape=(
            pltpu.VMEM((rows // m, full * m), f32),
            pltpu.VMEM((rows // m, full * m), f32),
            pltpu.VMEM((dim, full), bf16),
        ),
        in_specs=[pl.BlockSpec(memory_space=pl.ANY)] * 4,
        out_specs=(pl.BlockSpec(memory_space=pltpu.VMEM),) * 3,
        scratch_shapes=[
            pltpu.VMEM((a, b, tok, rows) if direct else (16, 128), bf16),
            pltpu.VMEM((a, rows, b * tok), bf16),
            pltpu.VMEM((nc, b * tok, cc), bf16),
            pltpu.VMEM((nc, rows, cc), f32),
            pltpu.VMEM((nc, rows, cc), f32),
            pltpu.VMEM((nc, rows, cc), bf16),
            pltpu.VMEM((rows, cc), f32),
            pltpu.VMEM((2, nc, a, rows, cc), bf16),
            pltpu.VMEM((nc, a, rows, cc), bf16),
            dma((a,)),
            dma((a, b)),
            dma((a, b)),
            dma((a, b, m)),
            dma((a, b, m)),
            dma((2, nc, b)),
            dma((3, nc)),
            dma((nc, a)),
            dma((2, nc, a)),
            dma((2, nc, a, columns)),
            dma((2, nc, a, columns)),
            dma((nc, a, b)),
            dma((nc, a, b)),
            dma((nc, 2, m)),
            dma((nc, 2, m)),
            dma((nc, 3)),
        ],
        compiler_params=pltpu.CompilerParams(
            collective_id=0, has_side_effects=True, vmem_limit_bytes=48 * 1024 * 1024),
        cost_estimate=pl.CostEstimate(flops=flops, bytes_accessed=4 * dim * full, transcendentals=rows * full),
    )(patches if direct else patches.T, cotangent, weight, accum)


def solution(mesh):
    return jax.shard_map(
        functools.partial(shards, mesh.shape["dp"], mesh.shape["mp"]),
        mesh=mesh,
        in_specs=(P("dp", None), P("dp", "mp"), P("dp", "mp"), P("dp", "mp")),
        out_specs=(P(("dp", "mp"), None), P(("dp", "mp"), None), P(None, "mp")),
        check_vma=False,
    )
```

```python
import functools

import jax
import jax.numpy as jnp
from jax import lax
from jax.experimental import pallas as pl
from jax.experimental.pallas import tpu as pltpu
from jax.sharding import PartitionSpec as P

learning_rate = 0.02
largest_product = 0.5625
power = 7
sum_lag, own_lag, copy_lag, end_lag, cross_lag = 1, 0, 1, 0, 4


def kernel(a, b, m, nc, direct, crossing, scale, p_ref, t_ref, w_ref, s_ref, ow_ref, os_ref, oc_ref,
           pv, pt, tv, wv, sv, gv, rbuf, sbuf,
           fown, fsend, frecv, qsend, qrecv, tsend, trecv, lsem, rsend, rrecv,
           csend, crecv, esend, erecv, osend, xsend, xrecv, yrecv, msend, mrecv):
    rows, full = w_ref.shape
    cc = full // nc
    tok = tv.shape[0] // b
    part_tok = tok // m
    sub = rows // m
    me = lax.axis_index("dp")
    mi = lax.axis_index("mp")
    zi = lax.div(me, b)
    xi = lax.rem(me, b)
    has_left = zi > 0
    has_right = zi < a - 1
    first_cross, step_cross, crossed = crossing

    def inner(j):
        return lax.rem(xi + j, b)

    def peer(j):
        return {"dp": zi * b + inner(j)}

    def other(j):
        return lax.rem(mi + j, m)

    left, right = {"dp": me - b}, {"dp": me + b}

    def remote(src, dst, send, recv, device):
        return pltpu.make_async_remote_copy(
            src_ref=src, dst_ref=dst, send_sem=send, recv_sem=recv,
            device_id=device, device_id_type=pl.DeviceIdType.MESH)

    def span(start, size):
        return pl.ds(pl.multiple_of(start, size), size)

    def cols(c):
        return span(c * cc, cc)

    def block(i):
        return span(i * rows, rows)

    def features(i, q=None):
        toks = slice(None) if q is None else span(q * part_tok, part_tok)
        return p_ref.at[toks, block(i)] if direct else p_ref.at[block(i), toks]

    def gathered(d, x, q=None):
        if direct:
            return pv.at[d, x] if q is None else pv.at[d, x, span(q * part_tok, part_tok)]
        return pt.at[d, :, span(x * tok, tok)] if q is None else pt.at[d, :, span(x * tok + q * part_tok, part_tok)]

    def own_features(d):
        return pltpu.make_async_copy(features(d * b + xi), gathered(d, xi), fown.at[d])

    def send_features(d, j):
        return remote(features(d * b + inner(j), mi), gathered(d, xi, mi), fsend.at[j - 1], frecv.at[d, j - 1], peer(j))

    def recv_features(d, j):
        spot = gathered(d, inner(b - j), mi)
        return remote(spot, spot, fsend.at[j - 1], frecv.at[d, j - 1], peer(j))

    def relay_features(d, j, k):
        spot = gathered(d, inner(b - j), mi)
        return remote(spot, spot, qsend.at[j - 1], qrecv.at[d, j - 1], {"mp": other(k)})

    def relayed(d, j):
        size = (m - 1) * part_tok
        spot = pv.at[d, 0, :size] if direct else pt.at[d, :, :size]
        return remote(spot, spot, qsend.at[j - 1], qrecv.at[d, j - 1], {"mp": other(1)})

    def sent_features(times):
        size = times * part_tok
        return p_ref.at[:size, :a * rows] if direct else p_ref.at[:a * rows, :size]

    def own(k):
        src, dst = ((t_ref, tv.at[span(xi * tok, tok)]), (w_ref, wv), (s_ref, sv))[k]
        return pltpu.make_async_copy(src, dst, lsem.at[k])

    def tokens(c, x):
        return tv.at[span(x * tok, tok), cols(c)]

    def send_tokens(c, j):
        return remote(t_ref.at[:, cols(c)], tokens(c, xi), tsend.at[j - 1], trecv.at[c, j - 1], peer(j))

    def recv_tokens(c, j):
        spot = tokens(c, inner(b - j))
        return remote(spot, spot, tsend.at[j - 1], trecv.at[c, j - 1], peer(j))

    def pass_sum(side, c, d):
        return remote(sbuf.at[c, d], rbuf.at[side, c, d], rsend.at[0], rrecv.at[side, c, d - 1 + side],
                      right if side == 0 else left)

    def region(owner, c):
        return oc_ref.at[block(owner), cols(c)]

    def pass_copy(side, c, h, owner_z):
        spot = region(owner_z * b + xi, c)
        return remote(spot, spot, csend.at[side, h], crecv.at[side, c, h], right if side == 0 else left)

    def pass_crossed(side, c, h, owner_z, j):
        spot = region(owner_z * b + inner(j), c)
        return remote(spot, spot, esend.at[side, h, j - 1], erecv.at[side, cross_index(c), h, j - 1],
                      right if side == 0 else left)

    def own_share(c, j):
        spot = region(me, c)
        return remote(spot, spot, osend.at[j - 1], xrecv.at[zi, j - 1], peer(j))

    def own_cross(c, j):
        spot = region(me, c)
        return remote(spot, spot, osend.at[j - 1], yrecv.at[cross_index(c), j - 1], peer(j))

    def recv_cross(c, j):
        spot = region(zi * b + inner(b - j), c)
        return remote(spot, spot, osend.at[j - 1], yrecv.at[cross_index(c), j - 1], peer(j))

    def share_copy(c, z, j):
        spot = region(z * b + xi, c)
        return remote(spot, spot, xsend.at[z, j - 1], xrecv.at[z, j - 1], peer(j))

    def whole(n, z, send, recv):
        spot = oc_ref.at[block(z * b), :n * cc]
        return remote(spot, spot, send, recv, peer(1))

    def flat(k, device):
        return (ow_ref if k == 0 else os_ref).at[:, span(device * full, full)]

    def flat_chunk(k, device, c):
        return (ow_ref if k == 0 else os_ref).at[:, span(device * full + c * cc, cc)]

    def state(k, i, c):
        return (wv if k == 0 else sv).at[span(i * sub, sub), cols(c)]

    def send_flat(c, k, j):
        return remote(state(k, other(j), c), flat_chunk(k, mi, c), msend.at[k, j - 1], mrecv.at[k, j - 1],
                      {"mp": other(j)})

    def whole_flat(k, j):
        return remote(flat(k, other(m - j)), flat(k, other(m - j)), msend.at[k, j - 1], mrecv.at[k, j - 1],
                      {"mp": other(j)})

    def cross_index(c):
        return lax.div(c - first_cross, step_cross)

    def crosses(c):
        if not crossed:
            return c < 0
        return (c >= first_cross) & (lax.rem(c - first_cross + step_cross * nc, step_cross) == 0) & (
            c < first_cross + step_cross * crossed)

    def valid(c):
        return (c >= 0) & (c < nc)

    barrier = pltpu.get_barrier_semaphore()

    def greet(device):
        pl.semaphore_signal(barrier, inc=1, device_id=device, device_id_type=pl.DeviceIdType.MESH)

    for j in range(1, b):
        greet(peer(j))
    for j in range(1, m):
        greet({"mp": other(j)})
    pl.when(has_left)(lambda: greet(left))
    pl.when(has_right)(lambda: greet(right))

    for d in range(a):
        own_features(d).start()
    for k in range(3):
        own(k).start()

    pl.semaphore_wait(barrier, b - 1 + m - 1 + jnp.minimum(zi, 1) + jnp.minimum(a - 1 - zi, 1))

    ahead = a - 1 - zi
    left_first = zi > ahead

    def nth(k):
        rightward = jnp.where(left_first, k - zi, k)
        leftward = jnp.where(left_first, k, k - ahead)
        goes_left = jnp.where(left_first, k < zi, k >= ahead)
        return jnp.where(k == a - 1, zi, jnp.where(goes_left, leftward, a - 1 - rightward))

    def place(side, k):
        return k + (jnp.where(left_first, zi, 0) if side == 0 else jnp.where(left_first, 0, ahead))

    def start_features(k):
        for j in range(1, b):
            send_features(nth(k), j).start()

    def spread_features(k):
        for j in range(1, b):
            recv_features(nth(k), j).wait_recv()
            for q in range(1, m):
                relay_features(nth(k), j, q).start()

    def start_tokens(c):
        for j in range(1, b):
            send_tokens(c, j).start()

    start_features(0)
    start_tokens(0)
    pl.loop(1, a)(start_features)
    pl.loop(1, nc)(start_tokens)
    spread_features(0)
    own(0).wait()

    def features_here(k, d):
        pl.when(k + 1 < a)(lambda: spread_features(k + 1))
        own_features(d).wait()
        for j in range(1, b):
            relayed(d, j).wait_recv()
        if direct:
            for x in range(b):
                pt[d, :, x * tok:(x + 1) * tok] = pv[d, x].T

    def product(c, d):
        return jnp.dot(pt[d], tv[:, cols(c)], preferred_element_type=jnp.float32)

    def coded(v):
        v = v * scale
        square = v * v
        return (square * square * square * v).astype(jnp.bfloat16)

    def decoded(code):
        c = code.astype(jnp.float32)
        size = jnp.maximum(jnp.abs(c), 2.0 ** -126)
        return c * jnp.exp2(jnp.log2(size) * (1 / power - 1)) * (1 / scale)

    def stage_tokens(c):
        for j in range(1, b):
            recv_tokens(c, j).wait_recv()

    def stage_sums(side, c):
        count, fed = (ahead, has_left) if side == 0 else (zi, has_right)

        @pl.loop(0, count)
        def _(k):
            d = a - 1 - k if side == 0 else k
            pl.when(c == 0)(lambda: features_here(place(side, k), d))

            @pl.when(fed)
            def _():
                total = product(c, d)
                pass_sum(side, c, d).wait_recv()
                sbuf[c, d] = coded(total + decoded(rbuf[side, c, d]))

            @pl.when(jnp.logical_not(fed))
            def _():
                sbuf[c, d] = coded(product(c, d))

            pass_sum(side, c, d).start()

    def stage_update(c):
        @pl.when(c == 0)
        def _():
            features_here(a - 1, zi)
            own(1).wait()
            own(2).wait()

        gv[...] = product(c, zi)
        for side, there in ((0, has_left), (1, has_right)):
            @pl.when(there)
            def _(side=side):
                pass_sum(side, c, zi).wait_recv()
                gv[...] += decoded(rbuf[side, c, zi])
        grad = gv[...]
        summed = sv[:, cols(c)] + grad * grad
        weight = wv[:, cols(c)] - learning_rate * grad * lax.rsqrt(summed)
        oc_ref[block(me), cols(c)] = weight.astype(oc_ref.dtype)
        sv[:, cols(c)] = summed
        wv[:, cols(c)] = weight
        pl.when(has_right)(lambda: pass_copy(0, c, 0, zi).start())
        pl.when(has_left)(lambda: pass_copy(1, c, 0, zi).start())
        for j in range(1, b):
            if crossed:
                pl.when(crosses(c))(lambda: own_cross(c, j).start())
            pl.when(jnp.logical_not(crosses(c)))(lambda: own_share(c, j).start())
        for k in range(2):
            for j in range(1, m):
                send_flat(c, k, j).start()
            flat_chunk(k, mi, c)[...] = state(k, mi, c)[...]

    def stage_across(c):
        for j in range(1, b):
            recv_cross(c, b - j).wait_recv()
            pl.when(has_right)(lambda: pass_crossed(0, c, 0, zi, j).start())
            pl.when(has_left)(lambda: pass_crossed(1, c, 0, zi, j).start())

    def stage_copy(c, side, h, owner_z, further):
        pass_copy(side, c, h - 1, owner_z).wait_recv()
        if further:
            pass_copy(side, c, h, owner_z).start()

        @pl.when(jnp.logical_not(crosses(c)))
        def _():
            for j in range(1, b):
                share_copy(c, owner_z, j).start()

    def stage_crossed(c, side, h, owner_z, further):
        for j in range(1, b):
            pass_crossed(side, c, h - 1, owner_z, j).wait_recv()
            if further:
                pass_crossed(side, c, h, owner_z, j).start()

    def distance(z):
        return jnp.maximum(z, a - 1 - z) * sum_lag + own_lag

    steps = nc + 2 * (a - 1) * max(sum_lag, copy_lag) + own_lag + end_lag + (cross_lag if crossed else 0)

    @pl.loop(0, steps)
    def _(i):
        ready = i - jnp.minimum(zi, a - 1 - zi) * sum_lag
        pl.when(valid(ready))(lambda: stage_tokens(ready))
        going_right = i - zi * sum_lag
        pl.when(valid(going_right))(lambda: stage_sums(0, going_right))
        going_left = i - (a - 1 - zi) * sum_lag
        pl.when(valid(going_left))(lambda: stage_sums(1, going_left))
        mine = i - distance(zi)
        pl.when(valid(mine))(lambda: stage_update(mine))
        if crossed:
            before = mine - cross_lag
            pl.when(valid(before) & crosses(before))(lambda: stage_across(before))
        for h in range(1, a):
            for side in range(2):
                owner_z = zi - h if side == 0 else zi + h
                there = owner_z >= 0 if side == 0 else owner_z < a
                onward = has_right if side == 0 else has_left
                for further in (True, False):
                    here = there & (onward if further else jnp.logical_not(onward))
                    c = i - distance(owner_z) - h * copy_lag - (0 if further else end_lag)
                    pl.when(here & valid(c))(functools.partial(stage_copy, c, side, h, owner_z, further))
                    if crossed:
                        e = c - cross_lag
                        pl.when(here & valid(e) & crosses(e))(
                            functools.partial(stage_crossed, e, side, h, owner_z, further))

    straight = nc - crossed
    for j in range(1, b):
        remote(sent_features(1), sent_features(1), fsend.at[j - 1], frecv.at[0, j - 1], peer(j)).wait_send()
        remote(sent_features(m - 1), sent_features(m - 1), qsend.at[j - 1], frecv.at[0, j - 1], peer(j)).wait_send()
        remote(t_ref, t_ref, tsend.at[j - 1], trecv.at[0, j - 1], peer(j)).wait_send()
        whole(nc, 0, osend.at[j - 1], osend.at[j - 1]).wait_send()
        for z in range(a):
            pl.when(z != zi)(lambda: whole(straight, z, xsend.at[z, j - 1], xrecv.at[z, j - 1]).wait_send())
            whole(straight, z, xsend.at[z, j - 1], xrecv.at[z, j - 1]).wait_recv()
    remote(sbuf.at[:, :a - 1], sbuf.at[:, :a - 1], rsend.at[0], rsend.at[0], peer(1)).wait_send()
    for h in range(a - 1):
        for side, owned, further in ((0, zi >= h, has_right), (1, zi + h < a, has_left)):
            @pl.when(owned & further)
            def _():
                whole(nc, 0, csend.at[side, h], csend.at[side, h]).wait_send()
                if crossed:
                    for j in range(1, b):
                        whole(crossed, 0, esend.at[side, h, j - 1], esend.at[side, h, j - 1]).wait_send()
    for k in range(2):
        for j in range(1, m):
            whole_flat(k, j).wait_send()
            whole_flat(k, j).wait_recv()


def shards(n, m, patches, cotangent, weight, accum):
    a = 1
    while a * a < n:
        a *= 2
    b = n // a
    nc = 16 if b == 2 else 8
    crossing = (1, 2, 2) if b == 2 else (0, 1, 0)
    direct = weight.shape[0] % 128 == 0
    tok, dim = patches.shape
    rows, full = weight.shape
    cc = full // nc
    columns = b - 1 if crossing[2] else 1
    scale = 1.0
    while (2 * scale * largest_product * tok * n) ** power < 2.0 ** 125:
        scale *= 2
    while (scale * largest_product * tok * n) ** power >= 2.0 ** 125:
        scale /= 2
    f32, bf16 = jnp.float32, jnp.bfloat16
    dma = pltpu.SemaphoreType.DMA
    flops = 2 * tok * b * a * rows * full
    return pl.pallas_call(
        functools.partial(kernel, a, b, m, nc, direct, crossing, scale),
        out_shape=(
            pltpu.VMEM((rows // m, full * m), f32),
            pltpu.VMEM((rows // m, full * m), f32),
            pltpu.VMEM((dim, full), bf16),
        ),
        in_specs=[pl.BlockSpec(memory_space=pl.ANY)] * 4,
        out_specs=(pl.BlockSpec(memory_space=pltpu.VMEM),) * 3,
        scratch_shapes=[
            pltpu.VMEM((a, b, tok, rows) if direct else (16, 128), bf16),
            pltpu.VMEM((a, rows, b * tok), bf16),
            pltpu.VMEM((b * tok, full), bf16),
            pltpu.VMEM((rows, full), f32),
            pltpu.VMEM((rows, full), f32),
            pltpu.VMEM((rows, cc), f32),
            pltpu.VMEM((2, nc, a, rows, cc), bf16),
            pltpu.VMEM((nc, a, rows, cc), bf16),
            dma((a,)),
            dma((b - 1,)),
            dma((a, b - 1)),
            dma((b - 1,)),
            dma((a, b - 1)),
            dma((b - 1,)),
            dma((nc, b - 1)),
            dma((3,)),
            dma((1,)),
            dma((2, nc, a - 1)),
            dma((2, a - 1)),
            dma((2, nc, a - 1)),
            dma((2, a - 1, columns)),
            dma((2, max(crossing[2], 1), a - 1, columns)),
            dma((b - 1,)),
            dma((a, b - 1)),
            dma((a, b - 1)),
            dma((max(crossing[2], 1), b - 1)),
            dma((2, m - 1)),
            dma((2, m - 1)),
        ],
        compiler_params=pltpu.CompilerParams(
            collective_id=0, has_side_effects=True, vmem_limit_bytes=48 * 1024 * 1024),
        cost_estimate=pl.CostEstimate(flops=flops, bytes_accessed=4 * dim * full, transcendentals=rows * full),
    )(patches if direct else patches.T, cotangent, weight, accum)


def solution(mesh):
    return jax.shard_map(
        functools.partial(shards, mesh.shape["dp"], mesh.shape["mp"]),
        mesh=mesh,
        in_specs=(P("dp", None), P("dp", "mp"), P("dp", "mp"), P("dp", "mp")),
        out_specs=(P(("dp", "mp"), None), P(("dp", "mp"), None), P(None, "mp")),
        check_vma=False,
    )
```

```python
import functools

import jax
import jax.numpy as jnp
from jax import lax
from jax.experimental import pallas as pl
from jax.experimental.pallas import tpu as pltpu
from jax.sharding import PartitionSpec as P

learning_rate = 0.02
largest_product = 0.5625
power = 7
sum_lag, own_lag, copy_lag, end_lag, cross_lag, token_lead = 1, 0, 1, 3, 3, 6


def kernel(a, b, m, nc, direct, crossing, scale, p_ref, t_ref, w_ref, s_ref, ow_ref, os_ref, oc_ref,
           pv, pt, tv, wv, sv, gv, rbuf, sbuf,
           fown, fsend, frecv, qsend, qrecv, grecv, tsend, trecv, lsem, rsend, rrecv,
           csend, crecv, esend, erecv, osend, xsend, xrecv, yrecv, msend, mrecv):
    rows, full = w_ref.shape
    cc = full // nc
    tok = tv.shape[0] // b
    part_tok = tok // m
    sub = rows // m
    me = lax.axis_index("dp")
    mi = lax.axis_index("mp")
    zi = lax.div(me, b)
    xi = lax.rem(me, b)
    has_left = zi > 0
    has_right = zi < a - 1
    crossed = len(crossing[0] + crossing[1]) > 0
    cores = 2 if m % 2 == 0 else 1
    pairs = m // cores
    pair = lax.div(mi, cores)
    core = lax.rem(mi, cores)

    def inner(j):
        return lax.rem(xi + j, b)

    def peer(j):
        return {"dp": zi * b + inner(j)}

    def other(j):
        return lax.rem(mi + j, m)

    left, right = {"dp": me - b}, {"dp": me + b}

    def remote(src, dst, send, recv, device):
        return pltpu.make_async_remote_copy(
            src_ref=src, dst_ref=dst, send_sem=send, recv_sem=recv,
            device_id=device, device_id_type=pl.DeviceIdType.MESH)

    def span(start, size):
        return pl.ds(pl.multiple_of(start, size), size)

    def cols(c):
        return span(c * cc, cc)

    def block(i):
        return span(i * rows, rows)

    def features(i, q=None):
        toks = slice(None) if q is None else span(q * part_tok, part_tok)
        return p_ref.at[toks, block(i)] if direct else p_ref.at[block(i), toks]

    def gathered(d, x, q=None):
        if direct:
            return pv.at[d, x] if q is None else pv.at[d, x, span(q * part_tok, part_tok)]
        return pt.at[d, :, span(x * tok, tok)] if q is None else pt.at[d, :, span(x * tok + q * part_tok, part_tok)]

    def own_features(d):
        return pltpu.make_async_copy(features(d * b + xi), gathered(d, xi), fown.at[d])

    def send_features(d, j):
        return remote(features(d * b + inner(j), mi), gathered(d, xi, mi), fsend.at[j - 1], frecv.at[d, j - 1], peer(j))

    def recv_features(d, j):
        spot = gathered(d, inner(b - j), mi)
        return remote(spot, spot, fsend.at[j - 1], frecv.at[d, j - 1], peer(j))

    def mate(k):
        return pair * cores + lax.rem(core + k, cores)

    def across_pairs(k):
        return lax.rem(pair + k, pairs) * cores + core

    def relay_features(d, j, k):
        spot = gathered(d, inner(b - j), mi)
        return remote(spot, spot, qsend.at[j - 1], grecv.at[d, j - 1, k - 1], {"mp": across_pairs(k)})

    def recv_relay(d, j, k):
        spot = gathered(d, inner(b - j), across_pairs(pairs - k))
        return remote(spot, spot, qsend.at[j - 1], grecv.at[d, j - 1, k - 1], {"mp": across_pairs(k)})

    def hand_features(d, j, k, q):
        spot = gathered(d, inner(b - j), q)
        return remote(spot, spot, qsend.at[j - 1], qrecv.at[d, j - 1], {"mp": mate(k)})

    def handed(d, j):
        size = (cores - 1) * pairs * part_tok
        spot = pv.at[d, 0, :size] if direct else pt.at[d, :, :size]
        return remote(spot, spot, qsend.at[j - 1], qrecv.at[d, j - 1], {"mp": mate(1)})

    def sent_features(times):
        size = times * part_tok
        return p_ref.at[:size, :a * rows] if direct else p_ref.at[:a * rows, :size]

    def own(k):
        src, dst = ((t_ref, tv.at[span(xi * tok, tok)]), (w_ref, wv), (s_ref, sv))[k]
        return pltpu.make_async_copy(src, dst, lsem.at[k])

    def tokens(c, x):
        return tv.at[span(x * tok, tok), cols(c)]

    def send_tokens(c, j):
        return remote(t_ref.at[:, cols(c)], tokens(c, xi), tsend.at[j - 1], trecv.at[c, j - 1], peer(j))

    def recv_tokens(c, j):
        spot = tokens(c, inner(b - j))
        return remote(spot, spot, tsend.at[j - 1], trecv.at[c, j - 1], peer(j))

    def pass_sum(side, c, d):
        return remote(sbuf.at[c, d], rbuf.at[side, c, d], rsend.at[0], rrecv.at[side, c, d - 1 + side],
                      right if side == 0 else left)

    def region(owner, c):
        return oc_ref.at[block(owner), cols(c)]

    def pass_copy(side, c, h, owner_z):
        spot = region(owner_z * b + xi, c)
        return remote(spot, spot, csend.at[side, h], crecv.at[side, c, h], right if side == 0 else left)

    def pass_crossed(side, c, h, owner_z, j):
        spot = region(owner_z * b + inner(j), c)
        return remote(spot, spot, esend.at[side, h, j - 1], erecv.at[side, c, h, j - 1],
                      right if side == 0 else left)

    def own_share(c, j):
        spot = region(me, c)
        return remote(spot, spot, osend.at[j - 1], xrecv.at[zi, j - 1], peer(j))

    def own_cross(c, j):
        spot = region(me, c)
        return remote(spot, spot, osend.at[j - 1], yrecv.at[c, j - 1], peer(j))

    def recv_cross(c, j):
        spot = region(zi * b + inner(b - j), c)
        return remote(spot, spot, osend.at[j - 1], yrecv.at[c, j - 1], peer(j))

    def share_copy(c, z, j):
        spot = region(z * b + xi, c)
        return remote(spot, spot, xsend.at[z, j - 1], xrecv.at[z, j - 1], peer(j))

    def whole(n, z, send, recv):
        spot = oc_ref.at[block(z * b), :n * cc]
        return remote(spot, spot, send, recv, peer(1))

    def flat(k, device):
        return (ow_ref if k == 0 else os_ref).at[:, span(device * full, full)]

    def flat_chunk(k, device, c):
        return (ow_ref if k == 0 else os_ref).at[:, span(device * full + c * cc, cc)]

    def state(k, i, c):
        return (wv if k == 0 else sv).at[span(i * sub, sub), cols(c)]

    def send_flat(c, k, j):
        return remote(state(k, other(j), c), flat_chunk(k, mi, c), msend.at[k, j - 1], mrecv.at[k, j - 1],
                      {"mp": other(j)})

    def whole_flat(k, j):
        return remote(flat(k, other(m - j)), flat(k, other(m - j)), msend.at[k, j - 1], mrecv.at[k, j - 1],
                      {"mp": other(j)})

    def at_end(z):
        return (z == 0) | (z == a - 1)

    masks = [sum(2 ** c for c in chosen) for chosen in crossing]

    def crosses(c, z):
        return lax.shift_right_logical(jnp.where(at_end(z), masks[0], masks[1]), c) % 2 == 1

    def valid(c):
        return (c >= 0) & (c < nc)

    barrier = pltpu.get_barrier_semaphore()

    def greet(device):
        pl.semaphore_signal(barrier, inc=1, device_id=device, device_id_type=pl.DeviceIdType.MESH)

    for j in range(1, b):
        greet(peer(j))
    for j in range(1, m):
        greet({"mp": other(j)})
    pl.when(has_left)(lambda: greet(left))
    pl.when(has_right)(lambda: greet(right))

    for d in range(a):
        own_features(d).start()
    for k in range(3):
        own(k).start()

    pl.semaphore_wait(barrier, b - 1 + m - 1 + jnp.minimum(zi, 1) + jnp.minimum(a - 1 - zi, 1))

    ahead = a - 1 - zi
    left_first = zi > ahead

    def nth(k):
        rightward = jnp.where(left_first, k - zi, k)
        leftward = jnp.where(left_first, k, k - ahead)
        goes_left = jnp.where(left_first, k < zi, k >= ahead)
        return jnp.where(k == a - 1, zi, jnp.where(goes_left, leftward, a - 1 - rightward))

    def place(side, k):
        return k + (jnp.where(left_first, zi, 0) if side == 0 else jnp.where(left_first, 0, ahead))

    def start_features(k):
        for j in range(1, b):
            send_features(nth(k), j).start()

    def spread_features(k):
        for j in range(1, b):
            recv_features(nth(k), j).wait_recv()
            for q in range(1, pairs):
                relay_features(nth(k), j, q).start()
            for q in range(1, cores):
                hand_features(nth(k), j, q, mi).start()

    def hand_on_features(k):
        for j in range(1, b):
            for q in range(1, pairs):
                recv_relay(nth(k), j, q).wait_recv()
                for r in range(1, cores):
                    hand_features(nth(k), j, r, across_pairs(pairs - q)).start()

    def start_tokens(c):
        for j in range(1, b):
            send_tokens(c, j).start()

    start_features(0)
    start_tokens(0)
    pl.loop(1, a)(start_features)
    pl.loop(1, min(token_lead, nc))(start_tokens)
    spread_features(0)
    hand_on_features(0)
    if a > 1:
        spread_features(1)
    own(0).wait()

    def features_here(d):
        own_features(d).wait()
        if cores > 1:
            for j in range(1, b):
                handed(d, j).wait_recv()
        if direct:
            for x in range(b):
                pt[d, :, x * tok:(x + 1) * tok] = pv[d, x].T

    def fetch_features(k):
        pl.when(k + 2 < a)(lambda: spread_features(k + 2))
        pl.when(k + 1 < a)(lambda: hand_on_features(k + 1))

    def product(c, d):
        return jnp.dot(pt[d], tv[:, cols(c)], preferred_element_type=jnp.float32)

    def coded(v):
        v = v * scale
        square = v * v
        return (square * square * square * v).astype(jnp.bfloat16)

    def decoded(code):
        c = code.astype(jnp.float32)
        size = jnp.maximum(jnp.abs(c), 2.0 ** -126)
        return c * jnp.exp2(jnp.log2(size) * (1 / power - 1)) * (1 / scale)

    def stage_tokens(c):
        pl.when(c + token_lead < nc)(lambda: start_tokens(c + token_lead))
        for j in range(1, b):
            recv_tokens(c, j).wait_recv()

    def stage_sums(side, c):
        count, fed = (ahead, has_left) if side == 0 else (zi, has_right)

        @pl.loop(0, count)
        def _(k):
            d = a - 1 - k if side == 0 else k
            pl.when(c == 0)(lambda: features_here(d))

            @pl.when(fed)
            def _():
                total = product(c, d)
                pl.when(c == 0)(lambda: fetch_features(place(side, k)))
                pass_sum(side, c, d).wait_recv()
                sbuf[c, d] = coded(total + decoded(rbuf[side, c, d]))

            @pl.when(jnp.logical_not(fed))
            def _():
                sbuf[c, d] = coded(product(c, d))

            pass_sum(side, c, d).start()
            pl.when((c == 0) & jnp.logical_not(fed))(lambda: fetch_features(place(side, k)))

    def stage_update(c):
        @pl.when(c == 0)
        def _():
            features_here(zi)
            own(1).wait()
            own(2).wait()

        gv[...] = product(c, zi)
        for side, there in ((0, has_left), (1, has_right)):
            @pl.when(there)
            def _(side=side):
                pass_sum(side, c, zi).wait_recv()
                gv[...] += decoded(rbuf[side, c, zi])
        grad = gv[...]
        summed = sv[:, cols(c)] + grad * grad
        weight = wv[:, cols(c)] - learning_rate * grad * lax.rsqrt(summed)
        oc_ref[block(me), cols(c)] = weight.astype(oc_ref.dtype)
        sv[:, cols(c)] = summed
        wv[:, cols(c)] = weight
        pl.when(has_right)(lambda: pass_copy(0, c, 0, zi).start())
        pl.when(has_left)(lambda: pass_copy(1, c, 0, zi).start())
        for j in range(1, b):
            if crossed:
                pl.when(crosses(c, zi))(lambda: own_cross(c, j).start())
            pl.when(jnp.logical_not(crosses(c, zi)))(lambda: own_share(c, j).start())
        for k in range(2):
            for j in range(1, m):
                send_flat(c, k, j).start()
            flat_chunk(k, mi, c)[...] = state(k, mi, c)[...]

    def stage_across(c):
        for j in range(1, b):
            recv_cross(c, b - j).wait_recv()
            pl.when(has_right)(lambda: pass_crossed(0, c, 0, zi, j).start())
            pl.when(has_left)(lambda: pass_crossed(1, c, 0, zi, j).start())

    def stage_copy(c, side, h, owner_z, further):
        pass_copy(side, c, h - 1, owner_z).wait_recv()
        if further:
            pass_copy(side, c, h, owner_z).start()

        @pl.when(jnp.logical_not(crosses(c, owner_z)))
        def _():
            for j in range(1, b):
                share_copy(c, owner_z, j).start()

    def stage_crossed(c, side, h, owner_z, further):
        for j in range(1, b):
            pass_crossed(side, c, h - 1, owner_z, j).wait_recv()
            if further:
                pass_crossed(side, c, h, owner_z, j).start()

    def distance(z):
        return jnp.maximum(z, a - 1 - z) * sum_lag + own_lag

    steps = nc + 2 * (a - 1) * max(sum_lag, copy_lag) + own_lag + end_lag + (cross_lag if crossed else 0)

    @pl.loop(0, steps)
    def _(i):
        ready = i - jnp.minimum(zi, a - 1 - zi) * sum_lag
        pl.when(valid(ready))(lambda: stage_tokens(ready))
        going_right = i - zi * sum_lag
        pl.when(valid(going_right))(lambda: stage_sums(0, going_right))
        going_left = i - (a - 1 - zi) * sum_lag
        pl.when(valid(going_left))(lambda: stage_sums(1, going_left))
        mine = i - distance(zi)
        pl.when(valid(mine))(lambda: stage_update(mine))
        if crossed:
            before = mine - cross_lag

            @pl.when(valid(before))
            def _():
                pl.when(crosses(before, zi))(lambda: stage_across(before))


        for h in range(1, a):
            for side in range(2):
                owner_z = zi - h if side == 0 else zi + h
                there = owner_z >= 0 if side == 0 else owner_z < a
                onward = has_right if side == 0 else has_left
                for further in (True, False):
                    here = there & (onward if further else jnp.logical_not(onward))
                    c = i - distance(owner_z) - h * copy_lag - (0 if further else end_lag)
                    pl.when(here & valid(c))(functools.partial(stage_copy, c, side, h, owner_z, further))
                    if crossed:
                        e = c - cross_lag

                        @pl.when(here & valid(e))
                        def _(e=e, side=side, h=h, owner_z=owner_z, further=further):
                            pl.when(crosses(e, owner_z))(
                                lambda: stage_crossed(e, side, h, owner_z, further))

    for j in range(1, b):
        remote(sent_features(1), sent_features(1), fsend.at[j - 1], frecv.at[0, j - 1], peer(j)).wait_send()
        remote(sent_features(m - 1), sent_features(m - 1), qsend.at[j - 1], frecv.at[0, j - 1], peer(j)).wait_send()
        remote(t_ref, t_ref, tsend.at[j - 1], trecv.at[0, j - 1], peer(j)).wait_send()
        whole(nc, 0, osend.at[j - 1], osend.at[j - 1]).wait_send()
        for z in range(a):
            straight = nc - len(crossing[0 if z in (0, a - 1) else 1])
            pl.when(z != zi)(lambda: whole(straight, z, xsend.at[z, j - 1], xrecv.at[z, j - 1]).wait_send())
            whole(straight, z, xsend.at[z, j - 1], xrecv.at[z, j - 1]).wait_recv()
    remote(sbuf.at[:, :a - 1], sbuf.at[:, :a - 1], rsend.at[0], rsend.at[0], peer(1)).wait_send()
    for h in range(a - 1):
        for side, owner_z, onward in ((0, zi - h, has_right), (1, zi + h, has_left)):
            sent = onward & (owner_z >= 0) & (owner_z < a)
            pl.when(sent)(lambda: whole(nc, 0, csend.at[side, h], csend.at[side, h]).wait_send())
            for chosen, there in ((crossing[0], at_end(owner_z)), (crossing[1], jnp.logical_not(at_end(owner_z)))):
                if chosen:
                    @pl.when(sent & there)
                    def _():
                        for j in range(1, b):
                            spot = esend.at[side, h, j - 1]
                            whole(len(chosen), 0, spot, spot).wait_send()
    for k in range(2):
        for j in range(1, m):
            whole_flat(k, j).wait_send()
            whole_flat(k, j).wait_recv()


def leave(pieces, *refs):
    count = len(refs) // 2
    sems = refs[-1]
    copies = []
    for k, (src, dst) in enumerate(zip(refs[:count], refs[count:2 * count])):
        step = src.shape[0] // pieces
        for i in range(pieces):
            part = slice(i * step, (i + 1) * step)
            copies.append(pltpu.make_async_copy(src.at[part], dst.at[part], sems.at[k, i]))
    for copy in copies:
        copy.start()
    for copy in copies:
        copy.wait()


def placed(results):
    pieces = 4
    return pl.pallas_call(
        functools.partial(leave, pieces),
        out_shape=tuple(jax.ShapeDtypeStruct(r.shape, r.dtype) for r in results),
        in_specs=[pl.BlockSpec(memory_space=pltpu.VMEM)] * len(results),
        out_specs=(pl.BlockSpec(memory_space=pl.ANY),) * len(results),
        scratch_shapes=[pltpu.SemaphoreType.DMA((len(results), pieces))],
        compiler_params=pltpu.CompilerParams(vmem_limit_bytes=20 * 1024 * 1024),
    )(*results)


def shards(n, m, patches, cotangent, weight, accum):
    a = 1
    while a * a < n:
        a *= 2
    b = n // a
    nc = 16 if b == 2 else 8
    crossing = ((7, 9, 10, 11, 12, 15), (2, 15)) if b == 2 else ((), ())
    crossed = len(crossing[0] + crossing[1]) > 0
    pairs = m // 2 if m % 2 == 0 else m
    direct = weight.shape[0] % 128 == 0
    tok, dim = patches.shape
    rows, full = weight.shape
    cc = full // nc
    columns = b - 1 if crossing[0] + crossing[1] else 1
    scale = 1.0
    while (2 * scale * largest_product * tok * n) ** power < 2.0 ** 125:
        scale *= 2
    while (scale * largest_product * tok * n) ** power >= 2.0 ** 125:
        scale /= 2
    f32, bf16 = jnp.float32, jnp.bfloat16
    dma = pltpu.SemaphoreType.DMA
    flops = 2 * tok * b * a * rows * full
    results = pl.pallas_call(
        functools.partial(kernel, a, b, m, nc, direct, crossing, scale),
        out_shape=(
            pltpu.VMEM((rows // m, full * m), f32),
            pltpu.VMEM((rows // m, full * m), f32),
            pltpu.VMEM((dim, full), bf16),
        ),
        in_specs=[pl.BlockSpec(memory_space=pl.ANY)] * 4,
        out_specs=(pl.BlockSpec(memory_space=pltpu.VMEM),) * 3,
        scratch_shapes=[
            pltpu.VMEM((a, b, tok, rows) if direct else (16, 128), bf16),
            pltpu.VMEM((a, rows, b * tok), bf16),
            pltpu.VMEM((b * tok, full), bf16),
            pltpu.VMEM((rows, full), f32),
            pltpu.VMEM((rows, full), f32),
            pltpu.VMEM((rows, cc), f32),
            pltpu.VMEM((2, nc, a, rows, cc), bf16),
            pltpu.VMEM((nc, a, rows, cc), bf16),
            dma((a,)),
            dma((b - 1,)),
            dma((a, b - 1)),
            dma((b - 1,)),
            dma((a, b - 1)),
            dma((a, b - 1, max(pairs - 1, 1))),
            dma((b - 1,)),
            dma((nc, b - 1)),
            dma((3,)),
            dma((1,)),
            dma((2, nc, a - 1)),
            dma((2, a - 1)),
            dma((2, nc, a - 1)),
            dma((2, a - 1, columns)),
            dma((2, nc if crossed else 1, a - 1, columns)),
            dma((b - 1,)),
            dma((a, b - 1)),
            dma((a, b - 1)),
            dma((nc if crossed else 1, b - 1)),
            dma((2, m - 1)),
            dma((2, m - 1)),
        ],
        compiler_params=pltpu.CompilerParams(
            collective_id=0, has_side_effects=True, vmem_limit_bytes=48 * 1024 * 1024),
        cost_estimate=pl.CostEstimate(flops=flops, bytes_accessed=4 * dim * full, transcendentals=rows * full),
    )(patches if direct else patches.T, cotangent, weight, accum)
    return placed(results)


def solution(mesh):
    return jax.shard_map(
        functools.partial(shards, mesh.shape["dp"], mesh.shape["mp"]),
        mesh=mesh,
        in_specs=(P("dp", None), P("dp", "mp"), P("dp", "mp"), P("dp", "mp")),
        out_specs=(P(("dp", "mp"), None), P(("dp", "mp"), None), P(None, "mp")),
        check_vma=False,
    )
```

```python
import functools

import jax
import jax.numpy as jnp
from jax import lax
from jax.experimental import pallas as pl
from jax.experimental.pallas import tpu as pltpu
from jax.sharding import PartitionSpec as P

learning_rate = 0.02
largest_product = 0.5625
power = 7
sum_lag, own_lag, copy_lag, end_lag, cross_lag, token_lead = 1, 0, 1, 3, 3, 6


def kernel(a, b, m, nc, direct, crossing, scale, p_ref, t_ref, w_ref, s_ref, ow_ref, os_ref, oc_ref,
           pv, pt, tv, wv, sv, gv, rbuf, sbuf,
           fown, fsend, frecv, qsend, qrecv, grecv, tsend, trecv, lsem, rsend, rrecv,
           csend, crecv, esend, erecv, osend, xsend, xrecv, yrecv, msend, mrecv):
    rows, full = w_ref.shape
    cc = full // nc
    tok = tv.shape[0] // b
    part_tok = tok // m
    sub = rows // m
    me = lax.axis_index("dp")
    mi = lax.axis_index("mp")
    zi = lax.div(me, b)
    xi = lax.rem(me, b)
    has_left = zi > 0
    has_right = zi < a - 1
    crossed = len(crossing[0] + crossing[1]) > 0
    cores = 2 if m % 2 == 0 else 1
    pairs = m // cores
    pair = lax.div(mi, cores)
    core = lax.rem(mi, cores)

    def inner(j):
        return lax.rem(xi + j, b)

    def peer(j):
        return {"dp": zi * b + inner(j)}

    def other(j):
        return lax.rem(mi + j, m)

    left, right = {"dp": me - b}, {"dp": me + b}

    def remote(src, dst, send, recv, device):
        return pltpu.make_async_remote_copy(
            src_ref=src, dst_ref=dst, send_sem=send, recv_sem=recv,
            device_id=device, device_id_type=pl.DeviceIdType.MESH)

    def span(start, size):
        return pl.ds(pl.multiple_of(start, size), size)

    def cols(c):
        return span(c * cc, cc)

    def block(i):
        return span(i * rows, rows)

    def features(i, q=None):
        toks = slice(None) if q is None else span(q * part_tok, part_tok)
        return p_ref.at[toks, block(i)] if direct else p_ref.at[block(i), toks]

    def gathered(d, x, q=None):
        if direct:
            return pv.at[d, x] if q is None else pv.at[d, x, span(q * part_tok, part_tok)]
        return pt.at[d, :, span(x * tok, tok)] if q is None else pt.at[d, :, span(x * tok + q * part_tok, part_tok)]

    def own_features(d):
        return pltpu.make_async_copy(features(d * b + xi), gathered(d, xi), fown.at[d])

    def send_features(d, j):
        return remote(features(d * b + inner(j), mi), gathered(d, xi, mi), fsend.at[j - 1], frecv.at[d, j - 1], peer(j))

    def recv_features(d, j):
        spot = gathered(d, inner(b - j), mi)
        return remote(spot, spot, fsend.at[j - 1], frecv.at[d, j - 1], peer(j))

    def mate(k):
        return pair * cores + lax.rem(core + k, cores)

    def across_pairs(k):
        return lax.rem(pair + k, pairs) * cores + core

    def relay_features(d, j, k):
        spot = gathered(d, inner(b - j), mi)
        return remote(spot, spot, qsend.at[j - 1], grecv.at[d, j - 1, k - 1], {"mp": across_pairs(k)})

    def recv_relay(d, j, k):
        spot = gathered(d, inner(b - j), across_pairs(pairs - k))
        return remote(spot, spot, qsend.at[j - 1], grecv.at[d, j - 1, k - 1], {"mp": across_pairs(k)})

    def hand_features(d, j, k, q):
        spot = gathered(d, inner(b - j), q)
        return remote(spot, spot, qsend.at[j - 1], qrecv.at[d, j - 1], {"mp": mate(k)})

    def handed(d, j):
        size = (cores - 1) * pairs * part_tok
        spot = pv.at[d, 0, :size] if direct else pt.at[d, :, :size]
        return remote(spot, spot, qsend.at[j - 1], qrecv.at[d, j - 1], {"mp": mate(1)})

    def sent_features(times):
        size = times * part_tok
        return p_ref.at[:size, :a * rows] if direct else p_ref.at[:a * rows, :size]

    def own(k):
        src, dst = ((t_ref, tv.at[span(xi * tok, tok)]), (w_ref, wv), (s_ref, sv))[k]
        return pltpu.make_async_copy(src, dst, lsem.at[k])

    def tokens(c, x):
        return tv.at[span(x * tok, tok), cols(c)]

    def send_tokens(c, j):
        return remote(t_ref.at[:, cols(c)], tokens(c, xi), tsend.at[j - 1], trecv.at[c, j - 1], peer(j))

    def recv_tokens(c, j):
        spot = tokens(c, inner(b - j))
        return remote(spot, spot, tsend.at[j - 1], trecv.at[c, j - 1], peer(j))

    def pass_sum(side, c, d):
        return remote(sbuf.at[c, d], rbuf.at[side, c, d], rsend.at[0], rrecv.at[c, d + 1 - side],
                      right if side == 0 else left)

    def region(owner, c):
        return oc_ref.at[block(owner), cols(c)]

    def pass_copy(side, c, h, owner_z):
        spot = region(owner_z * b + xi, c)
        return remote(spot, spot, csend.at[side, h], crecv.at[c, owner_z - side], right if side == 0 else left)

    def pass_crossed(side, c, h, owner_z, j):
        spot = region(owner_z * b + inner(j), c)
        return remote(spot, spot, esend.at[side, h, j - 1], erecv.at[c, owner_z - side, j - 1],
                      right if side == 0 else left)

    def own_share(c, j):
        spot = region(me, c)
        return remote(spot, spot, osend.at[j - 1], xrecv.at[zi, j - 1], peer(j))

    def own_cross(c, j):
        spot = region(me, c)
        return remote(spot, spot, osend.at[j - 1], yrecv.at[c, j - 1], peer(j))

    def recv_cross(c, j):
        spot = region(zi * b + inner(b - j), c)
        return remote(spot, spot, osend.at[j - 1], yrecv.at[c, j - 1], peer(j))

    def share_copy(c, z, j):
        spot = region(z * b + xi, c)
        return remote(spot, spot, xsend.at[z, j - 1], xrecv.at[z, j - 1], peer(j))

    def whole(n, z, send, recv):
        spot = oc_ref.at[block(z * b), :n * cc]
        return remote(spot, spot, send, recv, peer(1))

    def flat(k, device):
        return (ow_ref if k == 0 else os_ref).at[:, span(device * full, full)]

    def flat_chunk(k, device, c):
        return (ow_ref if k == 0 else os_ref).at[:, span(device * full + c * cc, cc)]

    def state(k, i, c):
        return (wv if k == 0 else sv).at[span(i * sub, sub), cols(c)]

    def send_flat(c, k, j):
        return remote(state(k, other(j), c), flat_chunk(k, mi, c), msend.at[k, j - 1], mrecv.at[k, j - 1],
                      {"mp": other(j)})

    def whole_flat(k, j):
        return remote(flat(k, other(m - j)), flat(k, other(m - j)), msend.at[k, j - 1], mrecv.at[k, j - 1],
                      {"mp": other(j)})

    def at_end(z):
        return (z == 0) | (z == a - 1)

    masks = [sum(2 ** c for c in chosen) for chosen in crossing]

    def crosses(c, z):
        return lax.shift_right_logical(jnp.where(at_end(z), masks[0], masks[1]), c) % 2 == 1

    def valid(c):
        return (c >= 0) & (c < nc)

    barrier = pltpu.get_barrier_semaphore()

    def greet(device):
        pl.semaphore_signal(barrier, inc=1, device_id=device, device_id_type=pl.DeviceIdType.MESH)

    for j in range(1, b):
        greet(peer(j))
    for j in range(1, m):
        greet({"mp": other(j)})
    pl.when(has_left)(lambda: greet(left))
    pl.when(has_right)(lambda: greet(right))

    for d in range(a):
        own_features(d).start()
    for k in range(3):
        own(k).start()

    pl.semaphore_wait(barrier, b - 1 + m - 1 + jnp.minimum(zi, 1) + jnp.minimum(a - 1 - zi, 1))

    ahead = a - 1 - zi
    left_first = zi > ahead

    def nth(k):
        rightward = jnp.where(left_first, k - zi, k)
        leftward = jnp.where(left_first, k, k - ahead)
        goes_left = jnp.where(left_first, k < zi, k >= ahead)
        return jnp.where(k == a - 1, zi, jnp.where(goes_left, leftward, a - 1 - rightward))

    def place(side, k):
        return k + (jnp.where(left_first, zi, 0) if side == 0 else jnp.where(left_first, 0, ahead))

    def start_features(k):
        for j in range(1, b):
            send_features(nth(k), j).start()

    def spread_features(k):
        for j in range(1, b):
            recv_features(nth(k), j).wait_recv()
            for q in range(1, pairs):
                relay_features(nth(k), j, q).start()
            for q in range(1, cores):
                hand_features(nth(k), j, q, mi).start()

    def hand_on_features(k):
        for j in range(1, b):
            for q in range(1, pairs):
                recv_relay(nth(k), j, q).wait_recv()
                for r in range(1, cores):
                    hand_features(nth(k), j, r, across_pairs(pairs - q)).start()

    def start_tokens(c):
        for j in range(1, b):
            send_tokens(c, j).start()

    start_features(0)
    start_tokens(0)
    pl.loop(1, a)(start_features)
    pl.loop(1, min(token_lead, nc))(start_tokens)
    spread_features(0)
    hand_on_features(0)
    if a > 1:
        spread_features(1)
    own(0).wait()

    def features_here(d):
        own_features(d).wait()
        if cores > 1:
            for j in range(1, b):
                handed(d, j).wait_recv()
        if direct:
            for x in range(b):
                pt[d, :, x * tok:(x + 1) * tok] = pv[d, x].T

    def fetch_features(k):
        pl.when(k + 2 < a)(lambda: spread_features(k + 2))
        pl.when(k + 1 < a)(lambda: hand_on_features(k + 1))

    def product(c, d):
        return jnp.dot(pt[d], tv[:, cols(c)], preferred_element_type=jnp.float32)

    def coded(v):
        v = v * scale
        square = v * v
        return (square * square * square * v).astype(jnp.bfloat16)

    def decoded(code):
        c = code.astype(jnp.float32)
        size = jnp.maximum(jnp.abs(c), 2.0 ** -126)
        return c * jnp.exp2(jnp.log2(size) * (1 / power - 1)) * (1 / scale)

    def stage_tokens(c):
        pl.when(c + token_lead < nc)(lambda: start_tokens(c + token_lead))
        for j in range(1, b):
            recv_tokens(c, j).wait_recv()

    def stage_sums(side, c):
        count, fed = (ahead, has_left) if side == 0 else (zi, has_right)

        @pl.loop(0, count)
        def _(k):
            d = a - 1 - k if side == 0 else k
            pl.when(c == 0)(lambda: features_here(d))

            @pl.when(fed)
            def _():
                total = product(c, d)
                pl.when(c == 0)(lambda: fetch_features(place(side, k)))
                pass_sum(side, c, d).wait_recv()
                sbuf[c, d] = coded(total + decoded(rbuf[side, c, d]))

            @pl.when(jnp.logical_not(fed))
            def _():
                sbuf[c, d] = coded(product(c, d))

            pass_sum(side, c, d).start()
            pl.when((c == 0) & jnp.logical_not(fed))(lambda: fetch_features(place(side, k)))

    def stage_update(c):
        @pl.when(c == 0)
        def _():
            features_here(zi)
            own(1).wait()
            own(2).wait()

        gv[...] = product(c, zi)
        for side, there in ((0, has_left), (1, has_right)):
            @pl.when(there)
            def _(side=side):
                pass_sum(side, c, zi).wait_recv()
                gv[...] += decoded(rbuf[side, c, zi])
        grad = gv[...]
        summed = sv[:, cols(c)] + grad * grad
        weight = wv[:, cols(c)] - learning_rate * grad * lax.rsqrt(summed)
        oc_ref[block(me), cols(c)] = weight.astype(oc_ref.dtype)
        sv[:, cols(c)] = summed
        wv[:, cols(c)] = weight
        pl.when(has_right)(lambda: pass_copy(0, c, 0, zi).start())
        pl.when(has_left)(lambda: pass_copy(1, c, 0, zi).start())
        for j in range(1, b):
            if crossed:
                pl.when(crosses(c, zi))(lambda: own_cross(c, j).start())
            pl.when(jnp.logical_not(crosses(c, zi)))(lambda: own_share(c, j).start())
        for k in range(2):
            for j in range(1, m):
                send_flat(c, k, j).start()
            flat_chunk(k, mi, c)[...] = state(k, mi, c)[...]

    def stage_across(c):
        for j in range(1, b):
            recv_cross(c, b - j).wait_recv()
            pl.when(has_right)(lambda: pass_crossed(0, c, 0, zi, j).start())
            pl.when(has_left)(lambda: pass_crossed(1, c, 0, zi, j).start())

    def stage_copy(c, side, h, owner_z, further):
        pass_copy(side, c, h - 1, owner_z).wait_recv()
        if further:
            pass_copy(side, c, h, owner_z).start()

        @pl.when(jnp.logical_not(crosses(c, owner_z)))
        def _():
            for j in range(1, b):
                share_copy(c, owner_z, j).start()

    def stage_crossed(c, side, h, owner_z, further):
        for j in range(1, b):
            pass_crossed(side, c, h - 1, owner_z, j).wait_recv()
            if further:
                pass_crossed(side, c, h, owner_z, j).start()

    def distance(z):
        return jnp.maximum(z, a - 1 - z) * sum_lag + own_lag

    steps = nc + 2 * (a - 1) * max(sum_lag, copy_lag) + own_lag + end_lag + (cross_lag if crossed else 0)

    @pl.loop(0, steps)
    def _(i):
        ready = i - jnp.minimum(zi, a - 1 - zi) * sum_lag
        pl.when(valid(ready))(lambda: stage_tokens(ready))
        going_right = i - zi * sum_lag
        going_left = i - (a - 1 - zi) * sum_lag
        early = jnp.logical_not(left_first)
        pl.when(valid(going_left) & early)(lambda: stage_sums(1, going_left))
        pl.when(valid(going_right))(lambda: stage_sums(0, going_right))
        pl.when(valid(going_left) & jnp.logical_not(early))(lambda: stage_sums(1, going_left))
        mine = i - distance(zi)
        pl.when(valid(mine))(lambda: stage_update(mine))
        if crossed:
            before = mine - cross_lag

            @pl.when(valid(before))
            def _():
                pl.when(crosses(before, zi))(lambda: stage_across(before))


        for h in range(1, a):
            for side in range(2):
                owner_z = zi - h if side == 0 else zi + h
                there = owner_z >= 0 if side == 0 else owner_z < a
                onward = has_right if side == 0 else has_left
                for further in (True, False):
                    here = there & (onward if further else jnp.logical_not(onward))
                    c = i - distance(owner_z) - h * copy_lag - (0 if further else end_lag)
                    pl.when(here & valid(c))(functools.partial(stage_copy, c, side, h, owner_z, further))
                    if crossed:
                        e = c - cross_lag

                        @pl.when(here & valid(e))
                        def _(e=e, side=side, h=h, owner_z=owner_z, further=further):
                            pl.when(crosses(e, owner_z))(
                                lambda: stage_crossed(e, side, h, owner_z, further))

    for j in range(1, b):
        remote(sent_features(1), sent_features(1), fsend.at[j - 1], frecv.at[0, j - 1], peer(j)).wait_send()
        remote(sent_features(m - 1), sent_features(m - 1), qsend.at[j - 1], frecv.at[0, j - 1], peer(j)).wait_send()
        remote(t_ref, t_ref, tsend.at[j - 1], trecv.at[0, j - 1], peer(j)).wait_send()
        whole(nc, 0, osend.at[j - 1], osend.at[j - 1]).wait_send()
        for z in range(a):
            straight = nc - len(crossing[0 if z in (0, a - 1) else 1])
            pl.when(z != zi)(lambda: whole(straight, z, xsend.at[z, j - 1], xrecv.at[z, j - 1]).wait_send())
            whole(straight, z, xsend.at[z, j - 1], xrecv.at[z, j - 1]).wait_recv()
    remote(sbuf.at[:, :a - 1], sbuf.at[:, :a - 1], rsend.at[0], rsend.at[0], peer(1)).wait_send()
    for h in range(a - 1):
        for side, owner_z, onward in ((0, zi - h, has_right), (1, zi + h, has_left)):
            sent = onward & (owner_z >= 0) & (owner_z < a)
            pl.when(sent)(lambda: whole(nc, 0, csend.at[side, h], csend.at[side, h]).wait_send())
            for chosen, there in ((crossing[0], at_end(owner_z)), (crossing[1], jnp.logical_not(at_end(owner_z)))):
                if chosen:
                    @pl.when(sent & there)
                    def _():
                        for j in range(1, b):
                            spot = esend.at[side, h, j - 1]
                            whole(len(chosen), 0, spot, spot).wait_send()
    for k in range(2):
        for j in range(1, m):
            whole_flat(k, j).wait_send()
            whole_flat(k, j).wait_recv()


def leave(pieces, *refs):
    count = len(refs) // 2
    sems = refs[-1]
    copies = []
    for k, (src, dst) in enumerate(zip(refs[:count], refs[count:2 * count])):
        step = src.shape[0] // pieces
        for i in range(pieces):
            part = slice(i * step, (i + 1) * step)
            copies.append(pltpu.make_async_copy(src.at[part], dst.at[part], sems.at[k, i]))
    for copy in copies:
        copy.start()
    for copy in copies:
        copy.wait()


def placed(results):
    pieces = 4
    return pl.pallas_call(
        functools.partial(leave, pieces),
        out_shape=tuple(jax.ShapeDtypeStruct(r.shape, r.dtype) for r in results),
        in_specs=[pl.BlockSpec(memory_space=pltpu.VMEM)] * len(results),
        out_specs=(pl.BlockSpec(memory_space=pl.ANY),) * len(results),
        scratch_shapes=[pltpu.SemaphoreType.DMA((len(results), pieces))],
        compiler_params=pltpu.CompilerParams(vmem_limit_bytes=20 * 1024 * 1024),
    )(*results)


def shards(n, m, patches, cotangent, weight, accum):
    a = 1
    while a * a < n:
        a *= 2
    b = n // a
    nc = 16 if b == 2 else 8
    crossing = ((7, 9, 10, 11, 12, 15), (2, 15)) if b == 2 else ((), ())
    crossed = len(crossing[0] + crossing[1]) > 0
    pairs = m // 2 if m % 2 == 0 else m
    direct = weight.shape[0] % 128 == 0
    tok, dim = patches.shape
    rows, full = weight.shape
    cc = full // nc
    columns = b - 1 if crossing[0] + crossing[1] else 1
    scale = 1.0
    while (2 * scale * largest_product * tok * n) ** power < 2.0 ** 125:
        scale *= 2
    while (scale * largest_product * tok * n) ** power >= 2.0 ** 125:
        scale /= 2
    f32, bf16 = jnp.float32, jnp.bfloat16
    dma = pltpu.SemaphoreType.DMA
    flops = 2 * tok * b * a * rows * full
    results = pl.pallas_call(
        functools.partial(kernel, a, b, m, nc, direct, crossing, scale),
        out_shape=(
            pltpu.VMEM((rows // m, full * m), f32),
            pltpu.VMEM((rows // m, full * m), f32),
            pltpu.VMEM((dim, full), bf16),
        ),
        in_specs=[pl.BlockSpec(memory_space=pl.ANY)] * 4,
        out_specs=(pl.BlockSpec(memory_space=pltpu.VMEM),) * 3,
        scratch_shapes=[
            pltpu.VMEM((a, b, tok, rows) if direct else (16, 128), bf16),
            pltpu.VMEM((a, rows, b * tok), bf16),
            pltpu.VMEM((b * tok, full), bf16),
            pltpu.VMEM((rows, full), f32),
            pltpu.VMEM((rows, full), f32),
            pltpu.VMEM((rows, cc), f32),
            pltpu.VMEM((2, nc, a, rows, cc), bf16),
            pltpu.VMEM((nc, a, rows, cc), bf16),
            dma((a,)),
            dma((b - 1,)),
            dma((a, b - 1)),
            dma((b - 1,)),
            dma((a, b - 1)),
            dma((a, b - 1, max(pairs - 1, 1))),
            dma((b - 1,)),
            dma((nc, b - 1)),
            dma((3,)),
            dma((1,)),
            dma((nc, a + 1)),
            dma((2, a - 1)),
            dma((nc, a - 1)),
            dma((2, a - 1, columns)),
            dma((nc if crossed else 1, a - 1, columns)),
            dma((b - 1,)),
            dma((a, b - 1)),
            dma((a, b - 1)),
            dma((nc if crossed else 1, b - 1)),
            dma((2, m - 1)),
            dma((2, m - 1)),
        ],
        compiler_params=pltpu.CompilerParams(
            collective_id=0, has_side_effects=True, vmem_limit_bytes=48 * 1024 * 1024),
        cost_estimate=pl.CostEstimate(flops=flops, bytes_accessed=4 * dim * full, transcendentals=rows * full),
    )(patches if direct else patches.T, cotangent, weight, accum)
    return placed(results)


def solution(mesh):
    return jax.shard_map(
        functools.partial(shards, mesh.shape["dp"], mesh.shape["mp"]),
        mesh=mesh,
        in_specs=(P("dp", None), P("dp", "mp"), P("dp", "mp"), P("dp", "mp")),
        out_specs=(P(("dp", "mp"), None), P(("dp", "mp"), None), P(None, "mp")),
        check_vma=False,
    )
```

```python
import functools

import jax
import jax.numpy as jnp
from jax import lax
from jax.experimental import pallas as pl
from jax.experimental.pallas import tpu as pltpu
from jax.sharding import PartitionSpec as P

learning_rate = 0.02
largest_product = 0.5625
power = 7
sum_lag, own_lag, copy_lag, end_lag, cross_lag, token_lead = 1, 0, 1, 2, 6, 9


def kernel(a, b, m, nc, direct, crossing, scale, p_ref, t_ref, w_ref, s_ref, ow_ref, os_ref, oc_ref,
           pv, pt, tv, wv, sv, gv, rbuf, sbuf,
           fown, fsend, frecv, qsend, qrecv, grecv, tsend, trecv, lsem, rsend, rrecv,
           csend, crecv, esend, erecv, osend, xsend, xrecv, yrecv, msend, mrecv):
    rows, full = w_ref.shape
    cc = full // nc
    tok = tv.shape[0] // b
    part_tok = tok // m
    sub = rows // m
    me = lax.axis_index("dp")
    mi = lax.axis_index("mp")
    zi = lax.div(me, b)
    xi = lax.rem(me, b)
    has_left = zi > 0
    has_right = zi < a - 1
    crossed = len(crossing[0] + crossing[1]) > 0
    cores = 2 if m % 2 == 0 else 1
    pairs = m // cores
    pair = lax.div(mi, cores)
    core = lax.rem(mi, cores)

    def inner(j):
        return lax.rem(xi + j, b)

    def peer(j):
        return {"dp": zi * b + inner(j)}

    def other(j):
        return lax.rem(mi + j, m)

    left, right = {"dp": me - b}, {"dp": me + b}

    def remote(src, dst, send, recv, device):
        return pltpu.make_async_remote_copy(
            src_ref=src, dst_ref=dst, send_sem=send, recv_sem=recv,
            device_id=device, device_id_type=pl.DeviceIdType.MESH)

    def span(start, size):
        return pl.ds(pl.multiple_of(start, size), size)

    def cols(c):
        return span(c * cc, cc)

    def block(i):
        return span(i * rows, rows)

    def features(i, q=None):
        toks = slice(None) if q is None else span(q * part_tok, part_tok)
        return p_ref.at[toks, block(i)] if direct else p_ref.at[block(i), toks]

    def gathered(d, x, q=None):
        if direct:
            return pv.at[d, x] if q is None else pv.at[d, x, span(q * part_tok, part_tok)]
        return pt.at[d, :, span(x * tok, tok)] if q is None else pt.at[d, :, span(x * tok + q * part_tok, part_tok)]

    def own_features(d):
        return pltpu.make_async_copy(features(d * b + xi), gathered(d, xi), fown.at[d])

    def send_features(d, j):
        return remote(features(d * b + inner(j), mi), gathered(d, xi, mi), fsend.at[j - 1], frecv.at[d, j - 1], peer(j))

    def recv_features(d, j):
        spot = gathered(d, inner(b - j), mi)
        return remote(spot, spot, fsend.at[j - 1], frecv.at[d, j - 1], peer(j))

    def mate(k):
        return pair * cores + lax.rem(core + k, cores)

    def across_pairs(k):
        return lax.rem(pair + k, pairs) * cores + core

    def relay_features(d, j, k):
        spot = gathered(d, inner(b - j), mi)
        return remote(spot, spot, qsend.at[j - 1], grecv.at[d, j - 1, k - 1], {"mp": across_pairs(k)})

    def recv_relay(d, j, k):
        spot = gathered(d, inner(b - j), across_pairs(pairs - k))
        return remote(spot, spot, qsend.at[j - 1], grecv.at[d, j - 1, k - 1], {"mp": across_pairs(k)})

    def hand_features(d, j, k, q):
        spot = gathered(d, inner(b - j), q)
        return remote(spot, spot, qsend.at[j - 1], qrecv.at[d, j - 1], {"mp": mate(k)})

    def handed(d, j):
        size = (cores - 1) * pairs * part_tok
        spot = pv.at[d, 0, :size] if direct else pt.at[d, :, :size]
        return remote(spot, spot, qsend.at[j - 1], qrecv.at[d, j - 1], {"mp": mate(1)})

    def sent_features(times):
        size = times * part_tok
        return p_ref.at[:size, :a * rows] if direct else p_ref.at[:a * rows, :size]

    def own(k):
        src, dst = ((t_ref, tv.at[span(xi * tok, tok)]), (w_ref, wv), (s_ref, sv))[k]
        return pltpu.make_async_copy(src, dst, lsem.at[k])

    def tokens(c, x):
        return tv.at[span(x * tok, tok), cols(c)]

    def send_tokens(c, j):
        return remote(t_ref.at[:, cols(c)], tokens(c, xi), tsend.at[j - 1], trecv.at[c, j - 1], peer(j))

    def recv_tokens(c, j):
        spot = tokens(c, inner(b - j))
        return remote(spot, spot, tsend.at[j - 1], trecv.at[c, j - 1], peer(j))

    def pass_sum(side, c, d):
        return remote(sbuf.at[c, d], rbuf.at[side, c, d], rsend.at[0], rrecv.at[c, d + 1 - side],
                      right if side == 0 else left)

    def region(owner, c):
        return oc_ref.at[block(owner), cols(c)]

    def pass_copy(side, c, h, owner_z):
        spot = region(owner_z * b + xi, c)
        return remote(spot, spot, csend.at[side, h], crecv.at[c, owner_z - side], right if side == 0 else left)

    def pass_crossed(side, c, h, owner_z, j):
        spot = region(owner_z * b + inner(j), c)
        return remote(spot, spot, esend.at[side, h, j - 1], erecv.at[rank(c), owner_z - side, j - 1],
                      right if side == 0 else left)

    def own_share(c, j):
        spot = region(me, c)
        return remote(spot, spot, osend.at[j - 1], xrecv.at[zi, j - 1], peer(j))

    def own_cross(c, j):
        spot = region(me, c)
        return remote(spot, spot, osend.at[j - 1], yrecv.at[rank(c), j - 1], peer(j))

    def recv_cross(c, j):
        spot = region(zi * b + inner(b - j), c)
        return remote(spot, spot, osend.at[j - 1], yrecv.at[rank(c), j - 1], peer(j))

    def share_copy(c, z, j):
        spot = region(z * b + xi, c)
        return remote(spot, spot, xsend.at[z, j - 1], xrecv.at[z, j - 1], peer(j))

    def whole(n, z, send, recv):
        spot = oc_ref.at[block(z * b), :n * cc]
        return remote(spot, spot, send, recv, peer(1))

    def flat(k, device):
        return (ow_ref if k == 0 else os_ref).at[:, span(device * full, full)]

    def flat_chunk(k, device, c):
        return (ow_ref if k == 0 else os_ref).at[:, span(device * full + c * cc, cc)]

    def state(k, i, c):
        return (wv if k == 0 else sv).at[span(i * sub, sub), cols(c)]

    def send_flat(c, k, j):
        return remote(state(k, other(j), c), flat_chunk(k, mi, c), msend.at[k, j - 1], mrecv.at[k, j - 1],
                      {"mp": other(j)})

    def whole_flat(k, j):
        return remote(flat(k, other(m - j)), flat(k, other(m - j)), msend.at[k, j - 1], mrecv.at[k, j - 1],
                      {"mp": other(j)})

    def at_end(z):
        return (z == 0) | (z == a - 1)

    masks = [sum(2 ** c for c in chosen) for chosen in crossing]

    def crosses(c, z):
        return lax.shift_right_logical(jnp.where(at_end(z), masks[0], masks[1]), c) % 2 == 1

    def rank(c):
        return sum((jnp.where(c > q, 1, 0) for q in sorted(set(crossing[0] + crossing[1]))), 0)

    def valid(c):
        return (c >= 0) & (c < nc)

    barrier = pltpu.get_barrier_semaphore()

    def greet(device):
        pl.semaphore_signal(barrier, inc=1, device_id=device, device_id_type=pl.DeviceIdType.MESH)

    for j in range(1, b):
        greet(peer(j))
    for j in range(1, m):
        greet({"mp": other(j)})
    pl.when(has_left)(lambda: greet(left))
    pl.when(has_right)(lambda: greet(right))

    for d in range(a):
        own_features(d).start()
    for k in range(3):
        own(k).start()

    pl.semaphore_wait(barrier, b - 1 + m - 1 + jnp.minimum(zi, 1) + jnp.minimum(a - 1 - zi, 1))

    ahead = a - 1 - zi
    left_first = zi > ahead

    def nth(k):
        rightward = jnp.where(left_first, k - zi, k)
        leftward = jnp.where(left_first, k, k - ahead)
        goes_left = jnp.where(left_first, k < zi, k >= ahead)
        return jnp.where(k == a - 1, zi, jnp.where(goes_left, leftward, a - 1 - rightward))

    def place(side, k):
        return k + (jnp.where(left_first, zi, 0) if side == 0 else jnp.where(left_first, 0, ahead))

    def start_features(k):
        for j in range(1, b):
            send_features(nth(k), j).start()

    def spread_features(k):
        for j in range(1, b):
            recv_features(nth(k), j).wait_recv()
            for q in range(1, pairs):
                relay_features(nth(k), j, q).start()
            for q in range(1, cores):
                hand_features(nth(k), j, q, mi).start()

    def hand_on_features(k):
        for j in range(1, b):
            for q in range(1, pairs):
                recv_relay(nth(k), j, q).wait_recv()
                for r in range(1, cores):
                    hand_features(nth(k), j, r, across_pairs(pairs - q)).start()

    def start_tokens(c):
        for j in range(1, b):
            send_tokens(c, j).start()

    start_features(0)
    start_tokens(0)
    pl.loop(1, a)(start_features)
    pl.loop(1, min(token_lead, nc))(start_tokens)
    spread_features(0)
    hand_on_features(0)
    if a > 1:
        spread_features(1)
    own(0).wait()

    def features_here(d):
        own_features(d).wait()
        if cores > 1:
            for j in range(1, b):
                handed(d, j).wait_recv()
        if direct:
            for x in range(b):
                pt[d, :, x * tok:(x + 1) * tok] = pv[d, x].T

    def fetch_features(k):
        pl.when(k + 2 < a)(lambda: spread_features(k + 2))
        pl.when(k + 1 < a)(lambda: hand_on_features(k + 1))

    def product(c, d):
        return jnp.dot(pt[d], tv[:, cols(c)], preferred_element_type=jnp.float32)

    def coded(v):
        v = v * scale
        square = v * v
        return (square * square * square * v).astype(jnp.bfloat16)

    def decoded(code):
        c = code.astype(jnp.float32)
        size = jnp.maximum(jnp.abs(c), 2.0 ** -126)
        return c * jnp.exp2(jnp.log2(size) * (1 / power - 1)) * (1 / scale)

    def stage_tokens(c):
        pl.when(c + token_lead < nc)(lambda: start_tokens(c + token_lead))
        for j in range(1, b):
            recv_tokens(c, j).wait_recv()

    def stage_sums(side, c):
        count, fed = (ahead, has_left) if side == 0 else (zi, has_right)

        @pl.loop(0, count)
        def _(k):
            d = a - 1 - k if side == 0 else k
            pl.when(c == 0)(lambda: features_here(d))

            @pl.when(fed)
            def _():
                total = product(c, d)
                pl.when(c == 0)(lambda: fetch_features(place(side, k)))
                pass_sum(side, c, d).wait_recv()
                sbuf[c, d] = coded(total + decoded(rbuf[side, c, d]))

            @pl.when(jnp.logical_not(fed))
            def _():
                sbuf[c, d] = coded(product(c, d))

            pass_sum(side, c, d).start()
            pl.when((c == 0) & jnp.logical_not(fed))(lambda: fetch_features(place(side, k)))

    def stage_update(c):
        @pl.when(c == 0)
        def _():
            features_here(zi)
            own(1).wait()
            own(2).wait()

        gv[...] = product(c, zi)
        for side, there in ((0, has_left), (1, has_right)):
            @pl.when(there)
            def _(side=side):
                pass_sum(side, c, zi).wait_recv()
                gv[...] += decoded(rbuf[side, c, zi])
        grad = gv[...]
        summed = sv[:, cols(c)] + grad * grad
        weight = wv[:, cols(c)] - learning_rate * grad * lax.rsqrt(summed)
        oc_ref[block(me), cols(c)] = weight.astype(oc_ref.dtype)
        sv[:, cols(c)] = summed
        wv[:, cols(c)] = weight
        pl.when(has_right)(lambda: pass_copy(0, c, 0, zi).start())
        pl.when(has_left)(lambda: pass_copy(1, c, 0, zi).start())
        for j in range(1, b):
            if crossed:
                pl.when(crosses(c, zi))(lambda: own_cross(c, j).start())
            pl.when(jnp.logical_not(crosses(c, zi)))(lambda: own_share(c, j).start())
        for k in range(2):
            for j in range(1, m):
                send_flat(c, k, j).start()
            flat_chunk(k, mi, c)[...] = state(k, mi, c)[...]

    def stage_across(c):
        for j in range(1, b):
            recv_cross(c, b - j).wait_recv()
            pl.when(has_right)(lambda: pass_crossed(0, c, 0, zi, j).start())
            pl.when(has_left)(lambda: pass_crossed(1, c, 0, zi, j).start())

    def stage_copy(c, side, h, owner_z, further):
        pass_copy(side, c, h - 1, owner_z).wait_recv()
        if further:
            pass_copy(side, c, h, owner_z).start()

        @pl.when(jnp.logical_not(crosses(c, owner_z)))
        def _():
            for j in range(1, b):
                share_copy(c, owner_z, j).start()

    def stage_crossed(c, side, h, owner_z, further):
        for j in range(1, b):
            pass_crossed(side, c, h - 1, owner_z, j).wait_recv()
            if further:
                pass_crossed(side, c, h, owner_z, j).start()

    def distance(z):
        return jnp.maximum(z, a - 1 - z) * sum_lag + own_lag

    steps = nc + 2 * (a - 1) * max(sum_lag, copy_lag) + own_lag + end_lag + (cross_lag if crossed else 0)

    @pl.loop(0, steps)
    def _(i):
        ready = i - jnp.minimum(zi, a - 1 - zi) * sum_lag
        pl.when(valid(ready))(lambda: stage_tokens(ready))
        going_right = i - zi * sum_lag
        going_left = i - (a - 1 - zi) * sum_lag
        early = jnp.logical_not(left_first)
        pl.when(valid(going_left) & early)(lambda: stage_sums(1, going_left))
        pl.when(valid(going_right))(lambda: stage_sums(0, going_right))
        pl.when(valid(going_left) & jnp.logical_not(early))(lambda: stage_sums(1, going_left))
        mine = i - distance(zi)
        pl.when(valid(mine))(lambda: stage_update(mine))
        if crossed:
            before = mine - cross_lag

            @pl.when(valid(before))
            def _():
                pl.when(crosses(before, zi))(lambda: stage_across(before))


        for h in range(1, a):
            for side in range(2):
                owner_z = zi - h if side == 0 else zi + h
                there = owner_z >= 0 if side == 0 else owner_z < a
                onward = has_right if side == 0 else has_left
                for further in (True, False):
                    here = there & (onward if further else jnp.logical_not(onward))
                    c = i - distance(owner_z) - h * copy_lag - (0 if further else end_lag)
                    pl.when(here & valid(c))(functools.partial(stage_copy, c, side, h, owner_z, further))
                    if crossed:
                        e = c - cross_lag

                        @pl.when(here & valid(e))
                        def _(e=e, side=side, h=h, owner_z=owner_z, further=further):
                            pl.when(crosses(e, owner_z))(
                                lambda: stage_crossed(e, side, h, owner_z, further))

    for j in range(1, b):
        remote(sent_features(1), sent_features(1), fsend.at[j - 1], frecv.at[0, j - 1], peer(j)).wait_send()
        remote(sent_features(m - 1), sent_features(m - 1), qsend.at[j - 1], frecv.at[0, j - 1], peer(j)).wait_send()
        remote(t_ref, t_ref, tsend.at[j - 1], trecv.at[0, j - 1], peer(j)).wait_send()
        whole(nc, 0, osend.at[j - 1], osend.at[j - 1]).wait_send()
        for z in range(a):
            straight = nc - len(crossing[0 if z in (0, a - 1) else 1])
            pl.when(z != zi)(lambda: whole(straight, z, xsend.at[z, j - 1], xrecv.at[z, j - 1]).wait_send())
            whole(straight, z, xsend.at[z, j - 1], xrecv.at[z, j - 1]).wait_recv()
    remote(sbuf.at[:, :a - 1], sbuf.at[:, :a - 1], rsend.at[0], rsend.at[0], peer(1)).wait_send()
    for h in range(a - 1):
        for side, owner_z, onward in ((0, zi - h, has_right), (1, zi + h, has_left)):
            sent = onward & (owner_z >= 0) & (owner_z < a)
            pl.when(sent)(lambda: whole(nc, 0, csend.at[side, h], csend.at[side, h]).wait_send())
            for chosen, there in ((crossing[0], at_end(owner_z)), (crossing[1], jnp.logical_not(at_end(owner_z)))):
                if chosen:
                    @pl.when(sent & there)
                    def _():
                        for j in range(1, b):
                            spot = esend.at[side, h, j - 1]
                            whole(len(chosen), 0, spot, spot).wait_send()
    for k in range(2):
        for j in range(1, m):
            whole_flat(k, j).wait_send()
            whole_flat(k, j).wait_recv()


def leave(pieces, *refs):
    count = len(refs) // 2
    sems = refs[-1]
    copies = []
    for k, (src, dst) in enumerate(zip(refs[:count], refs[count:2 * count])):
        step = src.shape[0] // pieces
        for i in range(pieces):
            part = slice(i * step, (i + 1) * step)
            copies.append(pltpu.make_async_copy(src.at[part], dst.at[part], sems.at[k, i]))
    for copy in copies:
        copy.start()
    for copy in copies:
        copy.wait()


def placed(results):
    pieces = 4
    return pl.pallas_call(
        functools.partial(leave, pieces),
        out_shape=tuple(jax.ShapeDtypeStruct(r.shape, r.dtype) for r in results),
        in_specs=[pl.BlockSpec(memory_space=pltpu.VMEM)] * len(results),
        out_specs=(pl.BlockSpec(memory_space=pl.ANY),) * len(results),
        scratch_shapes=[pltpu.SemaphoreType.DMA((len(results), pieces))],
        compiler_params=pltpu.CompilerParams(vmem_limit_bytes=20 * 1024 * 1024),
    )(*results)


def shards(n, m, patches, cotangent, weight, accum):
    a = 1
    while a * a < n:
        a *= 2
    b = n // a
    nc = 16 if b == 2 else 8
    crossing = ((4, 6, 8, 9, 10, 12), (6, 11)) if b == 2 else ((), ())
    crossed = len(set(crossing[0] + crossing[1]))
    pairs = m // 2 if m % 2 == 0 else m
    direct = weight.shape[0] % 128 == 0
    tok, dim = patches.shape
    rows, full = weight.shape
    cc = full // nc
    columns = b - 1 if crossing[0] + crossing[1] else 1
    scale = 1.0
    while (2 * scale * largest_product * tok * n) ** power < 2.0 ** 125:
        scale *= 2
    while (scale * largest_product * tok * n) ** power >= 2.0 ** 125:
        scale /= 2
    f32, bf16 = jnp.float32, jnp.bfloat16
    dma = pltpu.SemaphoreType.DMA
    flops = 2 * tok * b * a * rows * full
    results = pl.pallas_call(
        functools.partial(kernel, a, b, m, nc, direct, crossing, scale),
        out_shape=(
            pltpu.VMEM((rows // m, full * m), f32),
            pltpu.VMEM((rows // m, full * m), f32),
            pltpu.VMEM((dim, full), bf16),
        ),
        in_specs=[pl.BlockSpec(memory_space=pl.ANY)] * 4,
        out_specs=(pl.BlockSpec(memory_space=pltpu.VMEM),) * 3,
        scratch_shapes=[
            pltpu.VMEM((a, b, tok, rows) if direct else (16, 128), bf16),
            pltpu.VMEM((a, rows, b * tok), bf16),
            pltpu.VMEM((b * tok, full), bf16),
            pltpu.VMEM((rows, full), f32),
            pltpu.VMEM((rows, full), f32),
            pltpu.VMEM((rows, cc), f32),
            pltpu.VMEM((2, nc, a, rows, cc), bf16),
            pltpu.VMEM((nc, a, rows, cc), bf16),
            dma((a,)),
            dma((b - 1,)),
            dma((a, b - 1)),
            dma((b - 1,)),
            dma((a, b - 1)),
            dma((a, b - 1, max(pairs - 1, 1))),
            dma((b - 1,)),
            dma((nc, b - 1)),
            dma((3,)),
            dma((1,)),
            dma((nc, a + 1)),
            dma((2, a - 1)),
            dma((nc, a - 1)),
            dma((2, a - 1, columns)),
            dma((max(crossed, 1), a - 1, columns)),
            dma((b - 1,)),
            dma((a, b - 1)),
            dma((a, b - 1)),
            dma((max(crossed, 1), b - 1)),
            dma((2, m - 1)),
            dma((2, m - 1)),
        ],
        compiler_params=pltpu.CompilerParams(
            collective_id=0, has_side_effects=True, vmem_limit_bytes=48 * 1024 * 1024),
        cost_estimate=pl.CostEstimate(flops=flops, bytes_accessed=4 * dim * full, transcendentals=rows * full),
    )(patches if direct else patches.T, cotangent, weight, accum)
    return placed(results)


def solution(mesh):
    return jax.shard_map(
        functools.partial(shards, mesh.shape["dp"], mesh.shape["mp"]),
        mesh=mesh,
        in_specs=(P("dp", None), P("dp", "mp"), P("dp", "mp"), P("dp", "mp")),
        out_specs=(P(("dp", "mp"), None), P(("dp", "mp"), None), P(None, "mp")),
        check_vma=False,
    )
```
